8 devices in a mesh: dp: 2 (over z, y), ep: 4 (over x, core).
Axes of the slice: x: 2, y: 2, z: 1, core: 2. Of those that a mesh axis runs over, the one named last changes fastest.
Arguments:
- w_gate: bfloat16 [1, 8, 4096, 1536], P(None, 'ep')
- w_up: bfloat16 [1, 8, 4096, 1536], P(None, 'ep')
- w_down: bfloat16 [1, 8, 1536, 4096], P(None, 'ep')
- place: int32 [1, 32], replicated
Outputs:
- output 1: bfloat16 [1, 32, 4096, 3072], P(None, ('dp', 'ep'))
- output 2: bfloat16 [1, 32, 1536, 4096], P(None, ('dp', 'ep'))
All inputs are finite; a program needn't handle non-finite values.
Results may differ from the reference program's by a relative error of at most 0.001.
Values are sent between devices in bfloat16 or wider.
A program may use at most 1 GiB of HBM per device.

```python
import jax
import jax.numpy as jnp
import numpy as np

D = 4096
F = 1536
E = 8
L = 1
SLOTS = 4
DP = 2
EP = 4


def _slot_shard():
    n = np.arange(DP * EP)[:, None]
    j = np.arange(SLOTS)[None, :]
    a, g = n // EP, n % EP
    h = np.where(j < ((a + 1) * SLOTS) // DP, (2 * a - g) % EP, (g + j + 1) % EP)
    return h.reshape(-1)


def _draw_place(key):
    shard = E // EP
    width = DP * SLOTS

    def one(k):
        k1, k2, k3 = jax.random.split(k, 3)
        base = jax.random.permutation(k1, shard)
        extra = jax.random.randint(k2, (width - shard,), 0, shard)
        return jax.random.permutation(k3, jnp.concatenate([base, extra]))

    local = jax.vmap(one)(jax.random.split(key, L * EP)).reshape(L, EP, width)
    glob = (local + (jnp.arange(EP) * shard)[None, :, None]).reshape(L, EP * width)
    order = np.argsort(_slot_shard(), kind="stable")
    out = jnp.zeros((L, EP * width), jnp.int32).at[:, order].set(glob.astype(jnp.int32))
    return out


def setup_inputs(seed: int = 0) -> dict:
    kg, ku, kd, kp = jax.random.split(jax.random.PRNGKey(seed), 4)
    w_gate = jax.random.normal(kg, (L, E, D, F), jnp.float32).astype(jnp.bfloat16)
    w_up = jax.random.normal(ku, (L, E, D, F), jnp.float32).astype(jnp.bfloat16)
    w_down = jax.random.normal(kd, (L, E, F, D), jnp.float32).astype(jnp.bfloat16)
    return {"w_gate": w_gate, "w_up": w_up, "w_down": w_down, "place": _draw_place(kp)}


def reference(w_gate, w_up, w_down, place):
    take = jax.vmap(lambda w, i: w[i])
    w13 = jnp.concatenate([take(w_gate, place), take(w_up, place)], axis=-1)
    return w13, take(w_down, place)
```

```python
import functools

import jax
import jax.numpy as jnp
from jax import lax
from jax.experimental import pallas as pl
from jax.experimental.pallas import tpu as pltpu
from jax.sharding import PartitionSpec as P


TILE = 256
NBUF = 8
LAG = 3
DOWN = (768, 384, 192, 128, 64)


def _shard(dp, ep, slots, a, g, j):
    return (2 * a - g) % ep if j < ((a + 1) * slots) // dp else (g + j + 1) % ep


def _devices(dp, ep, slots, flip):
    return [[a * ep + g for a in range(dp) for g in range(ep) if _shard(dp, ep, slots, a, g, j) == g ^ flip]
            for j in range(slots)]


def _any(me, devices):
    hit = me < 0
    for n in sorted(set(devices)):
        hit = jnp.logical_or(hit, me == n)
    return hit


def _both(src, dests, experts, who, me, buf, rsem, wsem):
    rows = src.shape[1]
    tile = min(buf.shape[2], rows)
    steps = rows // tile
    nbuf = buf.shape[0]

    def read(t):
        return pltpu.make_async_copy(src.at[:, pl.ds(t * tile, tile)],
                                     buf.at[t % nbuf, :, pl.ds(0, tile)], rsem.at[t % nbuf])

    def writes(t, act):
        for j, dest in enumerate(dests):
            if who[j]:
                @pl.when(_any(me, who[j]))
                def _():
                    act(pltpu.make_async_copy(buf.at[t % nbuf, experts[j], pl.ds(0, tile)],
                                              dest(t * tile, tile), wsem.at[t % nbuf, j]))

    ahead = max(1, nbuf - LAG)
    for t in range(min(ahead, steps)):
        read(t).start()
    for t in range(steps):
        read(t).wait()
        writes(t, lambda c: c.start())
        n = t + ahead
        if n < steps:
            if n >= nbuf:
                writes(n - nbuf, lambda c: c.wait())
            read(n).start()
    for t in range(max(0, steps - nbuf), steps):
        writes(t, lambda c: c.wait())


def _one(src, expert, dest, buf, rsem, wsem):
    rows = src.shape[1]
    tile = min(buf.shape[2], rows)
    steps = rows // tile
    nbuf = buf.shape[0]

    def read(t):
        return pltpu.make_async_copy(src.at[expert, pl.ds(t * tile, tile)],
                                     buf.at[t % nbuf, 0, pl.ds(0, tile)], rsem.at[t % nbuf])

    def write(t):
        return pltpu.make_async_copy(buf.at[t % nbuf, 0, pl.ds(0, tile)],
                                     dest(t * tile, tile), wsem.at[t % nbuf, 0])

    ahead = max(1, nbuf - LAG)
    for t in range(min(ahead, steps)):
        read(t).start()
    for t in range(steps):
        read(t).wait()
        write(t).start()
        n = t + ahead
        if n < steps:
            if n >= nbuf:
                write(n - nbuf).wait()
            read(n).start()
    for t in range(max(0, steps - nbuf), steps):
        write(t).wait()


def solution(mesh):
    dp = mesh.shape["dp"]
    ep = mesh.shape["ep"]
    axes = ("dp", "ep")
    any_spec = pl.BlockSpec(memory_space=pltpu.HBM)
    smem_spec = pl.BlockSpec(memory_space=pltpu.SMEM)

    def hand_over(w_gate, w_up, w_down, place):
        wg, wu, wd = w_gate[0], w_up[0], w_down[0]
        n_exp, D, F = wg.shape
        slots = place.shape[1] // (dp * ep)
        own, across, beside, relayed = (_devices(dp, ep, slots, f) for f in (0, 2, 1, 3))
        to_x = [(n ^ 2, n) for n in sorted(set(sum(across, [])) | {m ^ 1 for m in sum(relayed, [])})]
        to_core = [(n ^ 1, n) for n in sorted(set(sum(beside, [])))]
        to_relay = [(n ^ 1, n) for n in sorted(set(sum(relayed, [])))]

        def scratch(cols, tile):
            return [pltpu.VMEM((NBUF, n_exp, tile, cols), jnp.bfloat16),
                    pltpu.SemaphoreType.DMA((NBUF,)), pltpu.SemaphoreType.DMA((NBUF, slots))]

        def where():
            return lax.axis_index("dp") * ep + lax.axis_index("ep")

        def half(out, j, k):
            return lambda r, n: out.at[j, pl.ds(r, n), pl.ds(k * F, F)]

        def rows_of(out, j, first):
            return lambda r, n: out.at[j, pl.ds(first + r, n)]

        def picks(place_ref, me):
            return [lax.rem(place_ref[0, me * slots + j], n_exp) for j in range(slots)]

        def first_kernel(place_ref, g, u, d, cg, cu, cd, o13, o2, buf_f, rf, wf, buf_d, rd, wd_):
            me = where()
            e = picks(place_ref, me)

            @pl.when(_any(me, sum(own, [])))
            def _():
                _both(g, [half(o13, j, 0) for j in range(slots)], e, own, me, buf_f, rf, wf)
                _both(u, [half(o13, j, 1) for j in range(slots)], e, own, me, buf_f, rf, wf)
                _both(d, [rows_of(o2, j, 0) for j in range(slots)], e, own, me, buf_d, rd, wd_)

            for j in range(slots):
                if beside[j]:
                    @pl.when(_any(me, beside[j]))
                    def _():
                        _one(cg, e[j], half(o13, j, 0), buf_f, rf, wf)
                        _one(cu, e[j], half(o13, j, 1), buf_f, rf, wf)
                        _one(cd, e[j], rows_of(o2, j, 0), buf_d, rd, wd_)

        def later_kernel(dest, place_ref, got, rel, _, out, buf, rs, ws):
            me = where()
            e = picks(place_ref, me)

            @pl.when(_any(me, sum(across, [])))
            def _():
                _both(got, [dest(out, j) for j in range(slots)], e, across, me, buf, rs, ws)

            for j in range(slots):
                if relayed[j]:
                    @pl.when(_any(me, relayed[j]))
                    def _():
                        _one(rel, e[j], dest(out, j), buf, rs, ws)

        o13_shape = jax.ShapeDtypeStruct((slots, D, 2 * F), jnp.bfloat16)
        o2_shape = jax.ShapeDtypeStruct((slots, F, D), jnp.bfloat16)

        def later(dest, got, rel, out, tile):
            size = got.size * got.dtype.itemsize
            return pl.pallas_call(
                functools.partial(later_kernel, dest),
                out_shape=jax.ShapeDtypeStruct(out.shape, out.dtype),
                in_specs=[smem_spec, any_spec, any_spec, any_spec], out_specs=any_spec,
                scratch_shapes=scratch(got.shape[2], tile),
                input_output_aliases={3: 0},
                cost_estimate=pl.CostEstimate(flops=0, bytes_accessed=3 * size, transcendentals=0),
            )(place, got, rel, out)

        def permute(x, pairs):
            return lax.ppermute(x, axes, pairs)

        got_g = permute(wg, to_x)
        got_u = permute(wu, to_x)
        pieces, r = [], 0
        for n in DOWN:
            pieces.append((r, permute(lax.slice_in_dim(wd, r, r + n, axis=1), to_x)))
            r += n
        side = [permute(w, to_core) for w in (wg, wu, wd)]
        own_bytes = 2 * 3 * wg.size * wg.dtype.itemsize
        w13, w2 = pl.pallas_call(
            first_kernel, name="place_own",
            out_shape=(o13_shape, o2_shape),
            in_specs=[smem_spec] + [any_spec] * 6, out_specs=(any_spec, any_spec),
            scratch_shapes=scratch(F, TILE) + scratch(D, TILE // 4),
            cost_estimate=pl.CostEstimate(flops=0, bytes_accessed=own_bytes, transcendentals=0),
        )(place, wg, wu, wd, *side)

        for k, got in enumerate((got_g, got_u)):
            w13 = later(functools.partial(lambda k, o, j: half(o, j, k), k),
                        got, permute(got, to_relay), w13, TILE)
        for r, got in pieces:
            w2 = later(functools.partial(lambda r, o, j: rows_of(o, j, r), r),
                       got, permute(got, to_relay), w2, min(TILE // 4, got.shape[1]))
        return w13[None], w2[None]

    spec_in = P(None, "ep", None, None)
    spec_out = P(None, ("dp", "ep"), None, None)
    return jax.shard_map(hand_over, mesh=mesh,
                         in_specs=(spec_in, spec_in, spec_in, P(None, None)),
                         out_specs=(spec_out, spec_out), check_vma=False)
```

```python
import functools

import jax
import jax.numpy as jnp
from jax import lax
from jax.experimental import pallas as pl
from jax.experimental.pallas import tpu as pltpu
from jax.sharding import PartitionSpec as P


TILE = 256
NBUF = 8
LAG = 3
VMEM_LIMIT = 32 * 1024 * 1024
BOTH_ROWS = 768
LAST_ROWS = (576, 128, 64)


def _shard(dp, ep, slots, a, g, j):
    return (2 * a - g) % ep if j < ((a + 1) * slots) // dp else (g + j + 1) % ep


def _devices(dp, ep, slots, flip):
    return [[a * ep + g for a in range(dp) for g in range(ep) if _shard(dp, ep, slots, a, g, j) == g ^ flip]
            for j in range(slots)]


def _any(me, devices):
    hit = me < 0
    for n in sorted(set(devices)):
        hit = jnp.logical_or(hit, me == n)
    return hit


def _stream(steps, nbuf, read, writes):
    ahead = max(1, nbuf - LAG)
    for t in range(min(ahead, steps)):
        read(t).start()
    for t in range(steps):
        read(t).wait()
        writes(t, lambda c: c.start())
        n = t + ahead
        if n < steps:
            if n >= nbuf:
                writes(n - nbuf, lambda c: c.wait())
            read(n).start()
    for t in range(max(0, steps - nbuf), steps):
        writes(t, lambda c: c.wait())


def _both(src, dests, experts, who, me, buf, rsem, wsem):
    rows, nbuf = src.shape[1], buf.shape[0]
    tile = min(buf.shape[2], rows)

    def read(t):
        return pltpu.make_async_copy(src.at[:, pl.ds(t * tile, tile)],
                                     buf.at[t % nbuf, :, pl.ds(0, tile)], rsem.at[t % nbuf])

    def writes(t, act):
        for j, dest in enumerate(dests):
            if who[j]:
                @pl.when(_any(me, who[j]))
                def _():
                    act(pltpu.make_async_copy(buf.at[t % nbuf, experts[j], pl.ds(0, tile)],
                                              dest(t * tile, tile), wsem.at[t % nbuf, j]))

    _stream(rows // tile, nbuf, read, writes)


def _one(src, dests, wanted, buf, rsem, wsem):
    rows, nbuf = src.shape[0], buf.shape[0]
    tile = min(buf.shape[2], rows)

    def read(t):
        return pltpu.make_async_copy(src.at[pl.ds(t * tile, tile)],
                                     buf.at[t % nbuf, 0, pl.ds(0, tile)], rsem.at[t % nbuf])

    def writes(t, act):
        for j, dest in enumerate(dests):
            def go():
                act(pltpu.make_async_copy(buf.at[t % nbuf, 0, pl.ds(0, tile)],
                                          dest(t * tile, tile), wsem.at[t % nbuf, j]))

            if wanted[j] is True:
                go()
            elif wanted[j] is not None:
                pl.when(wanted[j])(go)

    _stream(rows // tile, nbuf, read, writes)


def solution(mesh):
    dp = mesh.shape["dp"]
    ep = mesh.shape["ep"]
    axes = ("dp", "ep")
    hbm = pl.BlockSpec(memory_space=pltpu.HBM)
    vmem = pl.BlockSpec(memory_space=pltpu.VMEM)
    smem = pl.BlockSpec(memory_space=pltpu.SMEM)

    def hand_over(w_gate, w_up, w_down, place):
        wg, wu, wd = w_gate[0], w_up[0], w_down[0]
        n_exp, D, F = wg.shape
        slots = place.shape[1] // (dp * ep)
        own, across, beside, relayed = (_devices(dp, ep, slots, f) for f in (0, 2, 1, 3))
        to_x = [(n ^ 2, n) for n in sorted(set(sum(across, [])) | {m ^ 1 for m in sum(relayed, [])})]
        to_core = [(n ^ 1, n) for n in sorted(set(sum(beside, [])))]
        to_relay = [(n ^ 1, n) for n in sorted(set(sum(relayed, [])))]

        def ring(cols, tile, experts=n_exp):
            return [pltpu.VMEM((NBUF, experts, tile, cols), jnp.bfloat16),
                    pltpu.SemaphoreType.DMA((NBUF,)), pltpu.SemaphoreType.DMA((NBUF, slots))]

        def where():
            return lax.axis_index("dp") * ep + lax.axis_index("ep")

        def half(out, j, k):
            return lambda r, n: out.at[j, pl.ds(r, n), pl.ds(k * F, F)]

        def rows_of(out, j, first):
            return lambda r, n: out.at[j, pl.ds(first + r, n)]

        def picks(place_ref, me):
            return [lax.rem(place_ref[0, me * slots + j], n_exp) for j in range(slots)]

        def early(place_ref, me, flip):
            e = me * 0
            for j in range(slots):
                for n in relayed[j]:
                    e = jnp.where(me == n ^ flip, lax.rem(place_ref[0, n * slots + j], n_exp), e)
            return e

        def call(kernel, out_shape, in_specs, scratch, size, aliases=None):
            return pl.pallas_call(
                kernel, out_shape=out_shape, in_specs=in_specs,
                out_specs=jax.tree.map(lambda _: hbm, out_shape), scratch_shapes=scratch,
                input_output_aliases=aliases or {},
                compiler_params=pltpu.CompilerParams(vmem_limit_bytes=VMEM_LIMIT),
                cost_estimate=pl.CostEstimate(flops=0, bytes_accessed=size, transcendentals=0))

        def own_kernel(place_ref, g, u, d, cg, cu, cd, o13, o2, buf_f, rf, wf, buf_d, rd, wd_):
            me = where()
            e = picks(place_ref, me)

            @pl.when(_any(me, sum(own, [])))
            def _():
                _both(g, [half(o13, j, 0) for j in range(slots)], e, own, me, buf_f, rf, wf)
                _both(u, [half(o13, j, 1) for j in range(slots)], e, own, me, buf_f, rf, wf)
                _both(d, [rows_of(o2, j, 0) for j in range(slots)], e, own, me, buf_d, rd, wd_)

            for j in range(slots):
                if beside[j]:
                    @pl.when(_any(me, beside[j]))
                    def _():
                        _one(cg.at[e[j]], [half(o13, j, 0)], [True], buf_f, rf, wf)
                        _one(cu.at[e[j]], [half(o13, j, 1)], [True], buf_f, rf, wf)
                        _one(cd.at[e[j]], [rows_of(o2, j, 0)], [True], buf_d, rd, wd_)

        def both_kernel(dest, place_ref, got, rel, _, out, buf, rs, ws):
            me = where()
            e = picks(place_ref, me)

            @pl.when(_any(me, sum(across, [])))
            def _():
                _both(got, [dest(out, j) for j in range(slots)], e, across, me, buf, rs, ws)

            for j in range(slots):
                if relayed[j]:
                    @pl.when(_any(me, relayed[j]))
                    def _():
                        _one(rel.at[e[j]], [dest(out, j)], [True], buf, rs, ws)

        def wants(place_ref, me, first):
            e, a = picks(place_ref, me), early(place_ref, me, 1)
            return [jnp.logical_and(_any(me, across[j]), (e[j] == a) == first) if across[j] else None
                    for j in range(slots)]

        def first_kernel(dest, place_ref, got, rel, _, out, buf, rs, ws):
            me = where()

            @pl.when(_any(me, sum(across, [])))
            def _():
                _one(got, [dest(out, j) for j in range(slots)], wants(place_ref, me, True), buf, rs, ws)

            for j in range(slots):
                if relayed[j]:
                    @pl.when(_any(me, relayed[j]))
                    def _():
                        copy = pltpu.make_async_copy(rel, dest(out, j)(0, rel.shape[0]), rs.at[0])
                        copy.start()
                        copy.wait()

        def last_kernel(dest, place_ref, got, _, out, ws):
            want = wants(place_ref, where(), False)
            for act in (lambda c: c.start(), lambda c: c.wait()):
                for j in range(slots):
                    if want[j] is not None:
                        @pl.when(want[j])
                        def _():
                            act(pltpu.make_async_copy(got, dest(out, j)(0, got.shape[0]), ws.at[j]))

        def cut_kernel(place_ref, d, both, first, *rest):
            lasts, (buf, rs, ws) = rest[:-3], rest[-3:]
            e = early(place_ref, where(), 3)
            tile = buf.shape[2]
            steps = []
            for x in range(n_exp):
                for r in range(0, BOTH_ROWS, tile):
                    steps.append((d.at[x, pl.ds(r, tile)], both.at[x, pl.ds(r, tile)], tile))
            for ex, outs in ((e, [first]), (1 - e, lasts)):
                r = BOTH_ROWS
                for o in outs:
                    for q in range(0, o.shape[0], tile):
                        n = min(tile, o.shape[0] - q)
                        steps.append((d.at[ex, pl.ds(r + q, n)], o.at[pl.ds(q, n)], n))
                    r += o.shape[0]

            def read(t):
                return pltpu.make_async_copy(steps[t][0], buf.at[t % NBUF, 0, pl.ds(0, steps[t][2])], rs.at[t % NBUF])

            def writes(t, act):
                act(pltpu.make_async_copy(buf.at[t % NBUF, 0, pl.ds(0, steps[t][2])], steps[t][1], ws.at[t % NBUF, 0]))

            _stream(len(steps), NBUF, read, writes)

        def permute(x, pairs):
            return lax.ppermute(x, axes, pairs)

        def shape(*dims):
            return jax.ShapeDtypeStruct(dims, jnp.bfloat16)

        block = wg.size * wg.dtype.itemsize
        got_g = permute(wg, to_x)
        got_u = permute(wu, to_x)
        cuts = call(cut_kernel,
                    [shape(n_exp, BOTH_ROWS, D), shape(F - BOTH_ROWS, D)] + [shape(n, D) for n in LAST_ROWS],
                    [smem, hbm], ring(D, TILE // 2, 1), 2 * block)(place, wd)
        got_d = [permute(c, to_x) for c in cuts]
        side = [permute(w, to_core) for w in (wg, wu, wd)]
        w13, w2 = call(own_kernel, (shape(slots, D, 2 * F), shape(slots, F, D)),
                       [smem] + [hbm] * 6, ring(F, TILE) + ring(D, TILE // 4), 6 * block)(place, wg, wu, wd, *side)

        def later(kernel, dest, got, out, cols, tile, rel_in=hbm):
            rel = permute(got, to_relay)
            return call(functools.partial(kernel, dest), shape(*out.shape), [smem, hbm, rel_in, hbm],
                        ring(cols, tile), 3 * got.size * 2, {3: 0})(place, got, rel, out)

        w13 = later(both_kernel, lambda o, j: half(o, j, 0), got_g, w13, F, TILE)
        w13 = later(both_kernel, lambda o, j: half(o, j, 1), got_u, w13, F, TILE)
        w2 = later(both_kernel, lambda o, j: rows_of(o, j, 0), got_d[0], w2, D, TILE // 4)
        w2 = later(first_kernel, lambda o, j: rows_of(o, j, BOTH_ROWS), got_d[1], w2, D, TILE // 2,
                   vmem)
        r = BOTH_ROWS
        for got in got_d[2:]:
            w2 = call(functools.partial(last_kernel, lambda o, j, r=r: rows_of(o, j, r)),
                      shape(*w2.shape), [smem, vmem, hbm], [pltpu.SemaphoreType.DMA((slots,))],
                      3 * got.size * 2, {2: 0})(place, got, w2)
            r += got.shape[0]
        return w13[None], w2[None]

    spec_in = P(None, "ep", None, None)
    spec_out = P(None, ("dp", "ep"), None, None)
    return jax.shard_map(hand_over, mesh=mesh,
                         in_specs=(spec_in, spec_in, spec_in, P(None, None)),
                         out_specs=(spec_out, spec_out), check_vma=False)
```

```python
import functools

import jax
import jax.numpy as jnp
from jax import lax
from jax.experimental import pallas as pl
from jax.experimental.pallas import tpu as pltpu
from jax.sharding import PartitionSpec as P


TILE = 256
NBUF = 8
LAG = 3
VMEM_LIMIT = 32 * 1024 * 1024
BOTH_ROWS = 768
LAST_ROWS = (640, 96, 32)


def _shard(dp, ep, slots, a, g, j):
    return (2 * a - g) % ep if j < ((a + 1) * slots) // dp else (g + j + 1) % ep


def _devices(dp, ep, slots, flip):
    return [[a * ep + g for a in range(dp) for g in range(ep) if _shard(dp, ep, slots, a, g, j) == g ^ flip]
            for j in range(slots)]


def _any(me, devices):
    hit = me < 0
    for n in sorted(set(devices)):
        hit = jnp.logical_or(hit, me == n)
    return hit


def _stream(steps, nbuf, read, writes):
    ahead = max(1, nbuf - LAG)
    for t in range(min(ahead, steps)):
        read(t).start()
    for t in range(steps):
        read(t).wait()
        writes(t, lambda c: c.start())
        n = t + ahead
        if n < steps:
            if n >= nbuf:
                writes(n - nbuf, lambda c: c.wait())
            read(n).start()
    for t in range(max(0, steps - nbuf), steps):
        writes(t, lambda c: c.wait())


def _both(src, dests, experts, who, me, buf, rsem, wsem):
    rows, nbuf = src.shape[1], buf.shape[0]
    tile = min(buf.shape[2], rows)

    def read(t):
        return pltpu.make_async_copy(src.at[:, pl.ds(t * tile, tile)],
                                     buf.at[t % nbuf, :, pl.ds(0, tile)], rsem.at[t % nbuf])

    def writes(t, act):
        for j, dest in enumerate(dests):
            if who[j]:
                @pl.when(_any(me, who[j]))
                def _():
                    act(pltpu.make_async_copy(buf.at[t % nbuf, experts[j], pl.ds(0, tile)],
                                              dest(t * tile, tile), wsem.at[t % nbuf, j]))

    _stream(rows // tile, nbuf, read, writes)


def _one(src, dests, wanted, buf, rsem, wsem):
    rows, nbuf = src.shape[0], buf.shape[0]
    tile = min(buf.shape[2], rows)

    def read(t):
        return pltpu.make_async_copy(src.at[pl.ds(t * tile, tile)],
                                     buf.at[t % nbuf, 0, pl.ds(0, tile)], rsem.at[t % nbuf])

    def writes(t, act):
        for j, dest in enumerate(dests):
            def go():
                act(pltpu.make_async_copy(buf.at[t % nbuf, 0, pl.ds(0, tile)],
                                          dest(t * tile, tile), wsem.at[t % nbuf, j]))

            if wanted[j] is True:
                go()
            elif wanted[j] is not None:
                pl.when(wanted[j])(go)

    _stream(rows // tile, nbuf, read, writes)


def solution(mesh):
    dp = mesh.shape["dp"]
    ep = mesh.shape["ep"]
    axes = ("dp", "ep")
    hbm = pl.BlockSpec(memory_space=pltpu.HBM)
    vmem = pl.BlockSpec(memory_space=pltpu.VMEM)
    smem = pl.BlockSpec(memory_space=pltpu.SMEM)

    def hand_over(w_gate, w_up, w_down, place):
        wg, wu, wd = w_gate[0], w_up[0], w_down[0]
        n_exp, D, F = wg.shape
        slots = place.shape[1] // (dp * ep)
        own, across, beside, relayed = (_devices(dp, ep, slots, f) for f in (0, 2, 1, 3))
        to_x = [(n ^ 2, n) for n in sorted(set(sum(across, [])) | {m ^ 1 for m in sum(relayed, [])})]
        to_core = [(n ^ 1, n) for n in sorted(set(sum(beside, [])))]
        to_relay = [(n ^ 1, n) for n in sorted(set(sum(relayed, [])))]

        def ring(cols, tile, experts=n_exp):
            return [pltpu.VMEM((NBUF, experts, tile, cols), jnp.bfloat16),
                    pltpu.SemaphoreType.DMA((NBUF,)), pltpu.SemaphoreType.DMA((NBUF, slots))]

        def where():
            return lax.axis_index("dp") * ep + lax.axis_index("ep")

        def half(out, j, k):
            return lambda r, n: out.at[j, pl.ds(r, n), pl.ds(k * F, F)]

        def rows_of(out, j, first):
            return lambda r, n: out.at[j, pl.ds(first + r, n)]

        def picks(place_ref, me):
            return [lax.rem(place_ref[0, me * slots + j], n_exp) for j in range(slots)]

        def early(pick, me, flip):
            e = me * 0
            for _, n in to_x:
                on = [j for j in range(slots) if n ^ 1 in relayed[j]]
                here = [j for j in range(slots) if n in across[j]]
                if on:
                    first = pick(n ^ 1, on[0])
                else:
                    first = jnp.where(2 * sum(pick(n, j) for j in here) > len(here), 1, 0)
                e = jnp.where(me == n ^ flip, first, e)
            return e

        def scalars(place_ref):
            return lambda n, j: lax.rem(place_ref[0, n * slots + j], n_exp)

        def bits(place_ref):
            lane = lax.broadcasted_iota(jnp.int32, place_ref.shape, 1)
            mask = jnp.sum(jnp.left_shift(jnp.bitwise_and(place_ref[...], 1), lane))
            return lambda n, j: jnp.bitwise_and(jnp.right_shift(mask, n * slots + j), 1)

        def call(kernel, out_shape, in_specs, scratch, size, aliases=None):
            return pl.pallas_call(
                kernel, out_shape=out_shape, in_specs=in_specs,
                out_specs=jax.tree.map(lambda _: hbm, out_shape), scratch_shapes=scratch,
                input_output_aliases=aliases or {},
                compiler_params=pltpu.CompilerParams(vmem_limit_bytes=VMEM_LIMIT),
                cost_estimate=pl.CostEstimate(flops=0, bytes_accessed=size, transcendentals=0))

        def own_kernel(place_ref, g, u, d, cg, cu, cd, o13, o2, buf_f, rf, wf, buf_d, rd, wd_):
            me = where()
            e = picks(place_ref, me)

            @pl.when(_any(me, sum(own, [])))
            def _():
                _both(g, [half(o13, j, 0) for j in range(slots)], e, own, me, buf_f, rf, wf)
                _both(u, [half(o13, j, 1) for j in range(slots)], e, own, me, buf_f, rf, wf)
                _both(d, [rows_of(o2, j, 0) for j in range(slots)], e, own, me, buf_d, rd, wd_)

            for j in range(slots):
                if beside[j]:
                    @pl.when(_any(me, beside[j]))
                    def _():
                        _one(cg.at[e[j]], [half(o13, j, 0)], [True], buf_f, rf, wf)
                        _one(cu.at[e[j]], [half(o13, j, 1)], [True], buf_f, rf, wf)
                        _one(cd.at[e[j]], [rows_of(o2, j, 0)], [True], buf_d, rd, wd_)

        def both_kernel(dest, place_ref, got, rel, _, out, buf, rs, ws):
            me = where()
            e = picks(place_ref, me)

            @pl.when(_any(me, sum(across, [])))
            def _():
                _both(got, [dest(out, j) for j in range(slots)], e, across, me, buf, rs, ws)

            for j in range(slots):
                if relayed[j]:
                    @pl.when(_any(me, relayed[j]))
                    def _():
                        _one(rel.at[e[j]], [dest(out, j)], [True], buf, rs, ws)

        def wants(pick, me, first):
            a = early(pick, me, 0)
            return [jnp.logical_and(_any(me, across[j]), (pick(me, j) == a) == first) if across[j] else None
                    for j in range(slots)]

        def first_kernel(dest, place_ref, got, rel, _, out, buf, rs, ws):
            me = where()

            @pl.when(_any(me, sum(across, [])))
            def _():
                _one(got, [dest(out, j) for j in range(slots)], wants(scalars(place_ref), me, True), buf, rs, ws)

            for j in range(slots):
                if relayed[j]:
                    @pl.when(_any(me, relayed[j]))
                    def _():
                        copy = pltpu.make_async_copy(rel, dest(out, j)(0, rel.shape[0]), rs.at[0])
                        copy.start()
                        copy.wait()

        def last_kernel(dest, place_ref, got, _, out, ws):
            want = wants(bits(place_ref), where(), False)
            for act in (lambda c: c.start(), lambda c: c.wait()):
                for j in range(slots):
                    if want[j] is not None:
                        @pl.when(want[j])
                        def _():
                            act(pltpu.make_async_copy(got, dest(out, j)(0, got.shape[0]), ws.at[j]))

        def cut_kernel(place_ref, d, both, first, *rest):
            lasts, (buf, rs, ws) = rest[:-3], rest[-3:]
            e = early(scalars(place_ref), where(), 2)
            tile = buf.shape[2]
            steps = []
            for x in range(n_exp):
                for r in range(0, BOTH_ROWS, tile):
                    steps.append((d.at[x, pl.ds(r, tile)], both.at[x, pl.ds(r, tile)], tile))
            for ex, outs in ((e, [first]), (1 - e, lasts)):
                r = BOTH_ROWS
                for o in outs:
                    for q in range(0, o.shape[0], tile):
                        n = min(tile, o.shape[0] - q)
                        steps.append((d.at[ex, pl.ds(r + q, n)], o.at[pl.ds(q, n)], n))
                    r += o.shape[0]

            def read(t):
                return pltpu.make_async_copy(steps[t][0], buf.at[t % NBUF, 0, pl.ds(0, steps[t][2])], rs.at[t % NBUF])

            def writes(t, act):
                act(pltpu.make_async_copy(buf.at[t % NBUF, 0, pl.ds(0, steps[t][2])], steps[t][1], ws.at[t % NBUF, 0]))

            _stream(len(steps), NBUF, read, writes)

        def permute(x, pairs):
            return lax.ppermute(x, axes, pairs)

        def shape(*dims):
            return jax.ShapeDtypeStruct(dims, jnp.bfloat16)

        block = wg.size * wg.dtype.itemsize
        got_g = permute(wg, to_x)
        got_u = permute(wu, to_x)
        cuts = call(cut_kernel,
                    [shape(n_exp, BOTH_ROWS, D), shape(F - BOTH_ROWS, D)] + [shape(n, D) for n in LAST_ROWS],
                    [smem, hbm], ring(D, TILE // 2, 1), 2 * block)(place, wd)
        got_d = [permute(c, to_x) for c in cuts]
        side = [permute(w, to_core) for w in (wg, wu, wd)]
        w13, w2 = call(own_kernel, (shape(slots, D, 2 * F), shape(slots, F, D)),
                       [smem] + [hbm] * 6, ring(F, TILE) + ring(D, TILE // 4), 6 * block)(place, wg, wu, wd, *side)

        def later(kernel, dest, got, out, cols, tile, rel_in=hbm):
            rel = permute(got, to_relay)
            return call(functools.partial(kernel, dest), shape(*out.shape), [smem, hbm, rel_in, hbm],
                        ring(cols, tile), 3 * got.size * 2, {3: 0})(place, got, rel, out)

        w13 = later(both_kernel, lambda o, j: half(o, j, 0), got_g, w13, F, TILE)
        w13 = later(both_kernel, lambda o, j: half(o, j, 1), got_u, w13, F, TILE)
        w2 = later(both_kernel, lambda o, j: rows_of(o, j, 0), got_d[0], w2, D, TILE // 4)
        w2 = later(first_kernel, lambda o, j: rows_of(o, j, BOTH_ROWS), got_d[1], w2, D, TILE // 2,
                   vmem)
        r = BOTH_ROWS
        for got in got_d[2:]:
            w2 = call(functools.partial(last_kernel, lambda o, j, r=r: rows_of(o, j, r)),
                      shape(*w2.shape), [vmem, vmem, hbm], [pltpu.SemaphoreType.DMA((slots,))],
                      3 * got.size * 2, {2: 0})(place, got, w2)
            r += got.shape[0]
        return w13[None], w2[None]

    spec_in = P(None, "ep", None, None)
    spec_out = P(None, ("dp", "ep"), None, None)
    return jax.shard_map(hand_over, mesh=mesh,
                         in_specs=(spec_in, spec_in, spec_in, P(None, None)),
                         out_specs=(spec_out, spec_out), check_vma=False)
```

```python
import functools

import jax
import jax.numpy as jnp
from jax import lax
from jax.experimental import pallas as pl
from jax.experimental.pallas import tpu as pltpu
from jax.sharding import PartitionSpec as P


VMEM_LIMIT = 40 * 1024 * 1024
BOTH_ROWS = 768
LAST_ROWS = (672, 80, 16)
N_PIECES = 2 + len(LAST_ROWS)


def _shard(dp, ep, slots, a, g, j):
    return (2 * a - g) % ep if j < ((a + 1) * slots) // dp else (g + j + 1) % ep


def _devices(dp, ep, slots, flip):
    return [[a * ep + g for a in range(dp) for g in range(ep) if _shard(dp, ep, slots, a, g, j) == g ^ flip]
            for j in range(slots)]


def _any(me, devices):
    hit = me < 0
    for n in sorted(set(devices)):
        hit = jnp.logical_or(hit, me == n)
    return hit


def _place(src, buf, sem, dests, views, who, wsem):
    read = pltpu.make_async_copy(src, buf, sem)
    read.start()
    read.wait()
    for act in (lambda c: c.start(), lambda c: c.wait()):
        for j, dest in enumerate(dests):
            if who[j] is not None:
                @pl.when(who[j])
                def _():
                    act(pltpu.make_async_copy(views[j], dest, wsem.at[j]))


def solution(mesh):
    dp = mesh.shape["dp"]
    ep = mesh.shape["ep"]
    axes = ("dp", "ep")
    hbm = pl.BlockSpec(memory_space=pltpu.HBM)
    vmem = pl.BlockSpec(memory_space=pltpu.VMEM)
    smem = pl.BlockSpec(memory_space=pltpu.SMEM)

    def hand_over(w_gate, w_up, w_down, place):
        wg, wu, wd = w_gate[0], w_up[0], w_down[0]
        n_exp, D, F = wg.shape
        slots = place.shape[1] // (dp * ep)
        own, across, beside, relayed = (_devices(dp, ep, slots, f) for f in (0, 2, 1, 3))
        to_x = [(n ^ 2, n) for n in sorted(set(sum(across, [])) | {m ^ 1 for m in sum(relayed, [])})]
        to_core = [(n ^ 1, n) for n in sorted(set(sum(beside, [])))]
        to_relay = [(n ^ 1, n) for n in sorted(set(sum(relayed, [])))]

        def buffer(*dims):
            return [pltpu.VMEM(dims, jnp.bfloat16), pltpu.SemaphoreType.DMA, pltpu.SemaphoreType.DMA((slots,))]

        def where():
            return lax.axis_index("dp") * ep + lax.axis_index("ep")

        def half(out, j, k):
            return out.at[j, :, pl.ds(k * F, F)]

        def rows_of(out, j, first, n):
            return out.at[j, pl.ds(first, n)]

        def at(me, devices):
            return [_any(me, d) if d else None for d in devices]

        def picks(place_ref, me):
            return [lax.rem(place_ref[0, me * slots + j], n_exp) for j in range(slots)]

        def early(pick, me, flip):
            e = me * 0
            for _, n in to_x:
                on = [j for j in range(slots) if n ^ 1 in relayed[j]]
                here = [j for j in range(slots) if n in across[j]]
                if on:
                    first = pick(n ^ 1, on[0])
                else:
                    first = jnp.where(2 * sum(pick(n, j) for j in here) > len(here), 1, 0)
                e = jnp.where(me == n ^ flip, first, e)
            return e

        def scalars(place_ref):
            return lambda n, j: lax.rem(place_ref[0, n * slots + j], n_exp)

        def bits(place_ref):
            lane = lax.broadcasted_iota(jnp.int32, place_ref.shape, 1)
            mask = jnp.sum(jnp.left_shift(jnp.bitwise_and(place_ref[...], 1), lane))
            return lambda n, j: jnp.bitwise_and(jnp.right_shift(mask, n * slots + j), 1)

        def call(kernel, out_shape, in_specs, scratch, size, aliases=None):
            return pl.pallas_call(
                kernel, out_shape=out_shape, in_specs=in_specs,
                out_specs=jax.tree.map(lambda _: hbm, out_shape), scratch_shapes=scratch,
                input_output_aliases=aliases or {},
                compiler_params=pltpu.CompilerParams(vmem_limit_bytes=VMEM_LIMIT),
                cost_estimate=pl.CostEstimate(flops=0, bytes_accessed=size, transcendentals=0))

        def own_kernel(place_ref, g, u, d, cg, cu, cd, o13, o2, buf_f, sf, wf, buf_d, sd, wd_):
            me = where()
            e = picks(place_ref, me)
            n = buf_d.shape[1]
            for who, blocks in ((own, (g, u, d)), (beside, (cg, cu, cd))):
                @pl.when(_any(me, sum(who, [])))
                def _():
                    for k in range(2):
                        _place(blocks[k], buf_f, sf, [half(o13, j, k) for j in range(slots)],
                               [buf_f.at[e[j]] for j in range(slots)], at(me, who), wf)
                    for r in range(0, F, n):
                        _place(blocks[2].at[:, pl.ds(r, n)], buf_d, sd, [rows_of(o2, j, r, n) for j in range(slots)],
                               [buf_d.at[e[j]] for j in range(slots)], at(me, who), wd_)

        def both_kernel(dest, place_ref, got, rel, _, out, buf, sem, ws):
            me = where()
            e = picks(place_ref, me)
            for who, src in ((across, got), (relayed, rel)):
                @pl.when(_any(me, sum(who, [])))
                def _():
                    _place(src, buf, sem, [dest(out, j) for j in range(slots)],
                           [buf.at[e[j]] for j in range(slots)], at(me, who), ws)

        def wants(pick, me, first):
            a = early(pick, me, 0)
            return [jnp.logical_and(_any(me, across[j]), (pick(me, j) == a) == first) if across[j] else None
                    for j in range(slots)]

        def first_kernel(dest, place_ref, got, rel, _, out, buf, sem, ws):
            me = where()

            @pl.when(_any(me, sum(across, [])))
            def _():
                _place(got, buf, sem, [dest(out, j) for j in range(slots)], [buf] * slots,
                       wants(scalars(place_ref), me, True), ws)

            for j in range(slots):
                if relayed[j]:
                    @pl.when(_any(me, relayed[j]))
                    def _():
                        copy = pltpu.make_async_copy(rel, dest(out, j), sem)
                        copy.start()
                        copy.wait()

        def last_kernel(dest, place_ref, got, _, out, ws):
            want = wants(bits(place_ref), where(), False)
            for act in (lambda c: c.start(), lambda c: c.wait()):
                for j in range(slots):
                    if want[j] is not None:
                        @pl.when(want[j])
                        def _():
                            act(pltpu.make_async_copy(got, dest(out, j), ws.at[j]))

        def cut_kernel(place_ref, d, both, *rest):
            pieces, (buf, sem, ws) = rest[:-3], rest[-3:]
            e = early(scalars(place_ref), where(), 2)
            read = pltpu.make_async_copy(d, buf, sem)
            read.start()
            read.wait()
            writes = [pltpu.make_async_copy(buf.at[:, pl.ds(0, BOTH_ROWS)], both, ws.at[0])]
            r = BOTH_ROWS
            for i, o in enumerate(pieces):
                x = e if i == 0 else 1 - e
                writes.append(pltpu.make_async_copy(buf.at[x, pl.ds(r, o.shape[0])], o, ws.at[i + 1]))
                r = BOTH_ROWS if i == 0 else r + o.shape[0]
            for w in writes:
                w.start()
            for w in writes:
                w.wait()

        def permute(x, pairs):
            return lax.ppermute(x, axes, pairs)

        def shape(*dims):
            return jax.ShapeDtypeStruct(dims, jnp.bfloat16)

        block = wg.size * wg.dtype.itemsize
        got_g = permute(wg, to_x)
        got_u = permute(wu, to_x)
        cuts = call(cut_kernel,
                    [shape(n_exp, BOTH_ROWS, D), shape(F - BOTH_ROWS, D)] + [shape(n, D) for n in LAST_ROWS],
                    [smem, hbm], [pltpu.VMEM(wd.shape, jnp.bfloat16), pltpu.SemaphoreType.DMA,
                                  pltpu.SemaphoreType.DMA((N_PIECES,))], 2 * block)(place, wd)
        got_d = [permute(c, to_x) for c in cuts]
        side = [permute(w, to_core) for w in (wg, wu, wd)]
        w13, w2 = call(own_kernel, (shape(slots, D, 2 * F), shape(slots, F, D)),
                       [smem] + [hbm] * 6, buffer(*wg.shape) + buffer(n_exp, F // 2, D),
                       6 * block)(place, wg, wu, wd, *side)

        def later(kernel, dest, got, out, rel_in=hbm):
            rel = permute(got, to_relay)
            return call(functools.partial(kernel, dest), shape(*out.shape), [smem, hbm, rel_in, hbm],
                        buffer(*got.shape), 3 * got.size * 2, {3: 0})(place, got, rel, out)

        w13 = later(both_kernel, lambda o, j: half(o, j, 0), got_g, w13)
        w13 = later(both_kernel, lambda o, j: half(o, j, 1), got_u, w13)
        w2 = later(both_kernel, lambda o, j: rows_of(o, j, 0, BOTH_ROWS), got_d[0], w2)
        w2 = later(first_kernel, lambda o, j: rows_of(o, j, BOTH_ROWS, F - BOTH_ROWS), got_d[1], w2,
                   vmem)
        r = BOTH_ROWS
        for got in got_d[2:]:
            n = got.shape[0]
            w2 = call(functools.partial(last_kernel, lambda o, j, r=r, n=n: rows_of(o, j, r, n)),
                      shape(*w2.shape), [vmem, vmem, hbm], [pltpu.SemaphoreType.DMA((slots,))],
                      3 * got.size * 2, {2: 0})(place, got, w2)
            r += n
        return w13[None], w2[None]

    spec_in = P(None, "ep", None, None)
    spec_out = P(None, ("dp", "ep"), None, None)
    return jax.shard_map(hand_over, mesh=mesh,
                         in_specs=(spec_in, spec_in, spec_in, P(None, None)),
                         out_specs=(spec_out, spec_out), check_vma=False)
```

```python
import functools

import jax
import jax.numpy as jnp
from jax import lax
from jax.experimental import pallas as pl
from jax.experimental.pallas import tpu as pltpu
from jax.sharding import PartitionSpec as P


TILE = 512
NBUF = 4
VMEM_LIMIT = 40 * 1024 * 1024
BOTH_ROWS = 768
LAST_ROWS = (640, 112, 16)


def _shard(dp, ep, slots, a, g, j):
    return (2 * a - g) % ep if j < ((a + 1) * slots) // dp else (g + j + 1) % ep


def _devices(dp, ep, slots, flip):
    return [[a * ep + g for a in range(dp) for g in range(ep) if _shard(dp, ep, slots, a, g, j) == g ^ flip]
            for j in range(slots)]


def _any(me, devices):
    hit = me < 0
    for n in sorted(set(devices)):
        hit = jnp.logical_or(hit, me == n)
    return hit


def _tiles(rows, tile):
    out, r = [], 0
    for n in [tile // 8, tile // 4, tile - tile // 8 - tile // 4] + [tile] * rows:
        n = min(n, rows - r)
        if n:
            out.append((r, n))
        r += n
    return out


def _stream(steps, read, writes):
    for t in range(min(NBUF, steps)):
        read(t).start()
    for t in range(steps):
        read(t).wait()
        writes(t, lambda c: c.start())
        writes(t, lambda c: c.wait())
        if t + NBUF < steps:
            read(t + NBUF).start()


def _both(src, dests, experts, who, me, buf, rsem, wsem):
    tiles = _tiles(src.shape[1], buf.shape[2])

    def read(t):
        r, n = tiles[t]
        return pltpu.make_async_copy(src.at[:, pl.ds(r, n)], buf.at[t % NBUF, :, pl.ds(0, n)], rsem.at[t % NBUF])

    def writes(t, act):
        r, n = tiles[t]
        for j, dest in enumerate(dests):
            if who[j]:
                @pl.when(_any(me, who[j]))
                def _():
                    act(pltpu.make_async_copy(buf.at[t % NBUF, experts[j], pl.ds(0, n)], dest(r, n),
                                              wsem.at[t % NBUF, j]))

    _stream(len(tiles), read, writes)


def _one(src, dests, wanted, buf, rsem, wsem):
    tiles = _tiles(src.shape[0], buf.shape[2])

    def read(t):
        r, n = tiles[t]
        return pltpu.make_async_copy(src.at[pl.ds(r, n)], buf.at[t % NBUF, 0, pl.ds(0, n)], rsem.at[t % NBUF])

    def writes(t, act):
        r, n = tiles[t]
        for j, dest in enumerate(dests):
            def go():
                act(pltpu.make_async_copy(buf.at[t % NBUF, 0, pl.ds(0, n)], dest(r, n), wsem.at[t % NBUF, j]))

            if wanted[j] is True:
                go()
            elif wanted[j] is not None:
                pl.when(wanted[j])(go)

    _stream(len(tiles), read, writes)


def solution(mesh):
    dp = mesh.shape["dp"]
    ep = mesh.shape["ep"]
    axes = ("dp", "ep")
    hbm = pl.BlockSpec(memory_space=pltpu.HBM)
    vmem = pl.BlockSpec(memory_space=pltpu.VMEM)
    smem = pl.BlockSpec(memory_space=pltpu.SMEM)

    def hand_over(w_gate, w_up, w_down, place):
        wg, wu, wd = w_gate[0], w_up[0], w_down[0]
        n_exp, D, F = wg.shape
        slots = place.shape[1] // (dp * ep)
        own, across, beside, relayed = (_devices(dp, ep, slots, f) for f in (0, 2, 1, 3))
        to_x = [(n ^ 2, n) for n in sorted(set(sum(across, [])) | {m ^ 1 for m in sum(relayed, [])})]
        to_core = [(n ^ 1, n) for n in sorted(set(sum(beside, [])))]
        to_relay = [(n ^ 1, n) for n in sorted(set(sum(relayed, [])))]

        def ring(cols, tile, experts=n_exp):
            return [pltpu.VMEM((NBUF, experts, tile, cols), jnp.bfloat16),
                    pltpu.SemaphoreType.DMA((NBUF,)), pltpu.SemaphoreType.DMA((NBUF, slots))]

        def where():
            return lax.axis_index("dp") * ep + lax.axis_index("ep")

        def half(out, j, k):
            return lambda r, n: out.at[j, pl.ds(r, n), pl.ds(k * F, F)]

        def rows_of(out, j, first):
            return lambda r, n: out.at[j, pl.ds(first + r, n)]

        def picks(place_ref, me):
            return [lax.rem(place_ref[0, me * slots + j], n_exp) for j in range(slots)]

        def early(pick, me, flip):
            e = me * 0
            for _, n in to_x:
                on = [j for j in range(slots) if n ^ 1 in relayed[j]]
                here = [j for j in range(slots) if n in across[j]]
                if on:
                    first = pick(n ^ 1, on[0])
                else:
                    first = jnp.where(2 * sum(pick(n, j) for j in here) > len(here), 1, 0)
                e = jnp.where(me == n ^ flip, first, e)
            return e

        def scalars(place_ref):
            return lambda n, j: lax.rem(place_ref[0, n * slots + j], n_exp)

        def bits(place_ref):
            lane = lax.broadcasted_iota(jnp.int32, place_ref.shape, 1)
            mask = jnp.sum(jnp.left_shift(jnp.bitwise_and(place_ref[...], 1), lane))
            return lambda n, j: jnp.bitwise_and(jnp.right_shift(mask, n * slots + j), 1)

        def call(kernel, out_shape, in_specs, scratch, size, aliases=None):
            return pl.pallas_call(
                kernel, out_shape=out_shape, in_specs=in_specs,
                out_specs=jax.tree.map(lambda _: hbm, out_shape), scratch_shapes=scratch,
                input_output_aliases=aliases or {},
                compiler_params=pltpu.CompilerParams(vmem_limit_bytes=VMEM_LIMIT),
                cost_estimate=pl.CostEstimate(flops=0, bytes_accessed=size, transcendentals=0))

        def own_kernel(place_ref, g, u, d, cg, cu, cd, o13, o2, buf_f, rf, wf, buf_d, rd, wd_):
            me = where()
            e = picks(place_ref, me)

            many = [n for n in range(dp * ep) if sum(n in d for d in own) > 1]

            @pl.when(_any(me, many))
            def _():
                _both(g, [half(o13, j, 0) for j in range(slots)], e, own, me, buf_f, rf, wf)
                _both(u, [half(o13, j, 1) for j in range(slots)], e, own, me, buf_f, rf, wf)
                _both(d, [rows_of(o2, j, 0) for j in range(slots)], e, own, me, buf_d, rd, wd_)

            for who, blocks in ((own, (g, u, d)), (beside, (cg, cu, cd))):
                for j in range(slots):
                    single = [n for n in who[j] if who is beside or n not in many]
                    if single:
                        @pl.when(_any(me, single))
                        def _():
                            _one(blocks[0].at[e[j]], [half(o13, j, 0)], [True], buf_f, rf, wf)
                            _one(blocks[1].at[e[j]], [half(o13, j, 1)], [True], buf_f, rf, wf)
                            _one(blocks[2].at[e[j]], [rows_of(o2, j, 0)], [True], buf_d, rd, wd_)

        def both_kernel(dest, place_ref, got, rel, _, out, buf, rs, ws):
            me = where()
            e = picks(place_ref, me)

            @pl.when(_any(me, sum(across, [])))
            def _():
                _both(got, [dest(out, j) for j in range(slots)], e, across, me, buf, rs, ws)

            for j in range(slots):
                if relayed[j]:
                    @pl.when(_any(me, relayed[j]))
                    def _():
                        _one(rel.at[e[j]], [dest(out, j)], [True], buf, rs, ws)

        def wants(pick, me, first):
            a = early(pick, me, 0)
            return [jnp.logical_and(_any(me, across[j]), (pick(me, j) == a) == first) if across[j] else None
                    for j in range(slots)]

        def first_kernel(dest, place_ref, got, rel, _, out, buf, rs, ws):
            me = where()

            @pl.when(_any(me, sum(across, [])))
            def _():
                _one(got, [dest(out, j) for j in range(slots)], wants(scalars(place_ref), me, True), buf, rs, ws)

            for j in range(slots):
                if relayed[j]:
                    @pl.when(_any(me, relayed[j]))
                    def _():
                        copy = pltpu.make_async_copy(rel, dest(out, j)(0, rel.shape[0]), rs.at[0])
                        copy.start()
                        copy.wait()

        def other_kernel(dest, place_ref, got, _, out, buf, rs, ws):
            me = where()

            @pl.when(_any(me, sum(across, [])))
            def _():
                _one(got, [dest(out, j) for j in range(slots)], wants(scalars(place_ref), me, False), buf, rs, ws)

        def last_kernel(dest, place_ref, got, _, out, ws):
            want = wants(bits(place_ref), where(), False)
            for act in (lambda c: c.start(), lambda c: c.wait()):
                for j in range(slots):
                    if want[j] is not None:
                        @pl.when(want[j])
                        def _():
                            act(pltpu.make_async_copy(got, dest(out, j)(0, got.shape[0]), ws.at[j]))

        def cut_kernel(place_ref, d, both, *rest):
            pieces, (buf, rs, ws) = rest[:-3], rest[-3:]
            e = early(scalars(place_ref), where(), 2)
            tile = buf.shape[2]
            steps = [(d.at[x, pl.ds(r, n)], both.at[x, pl.ds(r, n)], n)
                     for x in range(n_exp) for r, n in _tiles(BOTH_ROWS, tile)]
            first = BOTH_ROWS
            for i, o in enumerate(pieces):
                x = e if i == 0 else 1 - e
                for r, n in _tiles(o.shape[0], tile):
                    steps.append((d.at[x, pl.ds(first + r, n)], o.at[pl.ds(r, n)], n))
                first = BOTH_ROWS if i == 0 else first + o.shape[0]

            def read(t):
                src, _, n = steps[t]
                return pltpu.make_async_copy(src, buf.at[t % NBUF, 0, pl.ds(0, n)], rs.at[t % NBUF])

            def writes(t, act):
                _, dst, n = steps[t]
                act(pltpu.make_async_copy(buf.at[t % NBUF, 0, pl.ds(0, n)], dst, ws.at[t % NBUF, 0]))

            _stream(len(steps), read, writes)

        def permute(x, pairs):
            return lax.ppermute(x, axes, pairs)

        def shape(*dims):
            return jax.ShapeDtypeStruct(dims, jnp.bfloat16)

        block = wg.size * wg.dtype.itemsize
        got_g = permute(wg, to_x)
        got_u = permute(wu, to_x)
        cuts = call(cut_kernel,
                    [shape(n_exp, BOTH_ROWS, D), shape(F - BOTH_ROWS, D)] + [shape(n, D) for n in LAST_ROWS],
                    [smem, hbm], ring(D, TILE // 2, 1), 2 * block)(place, wd)
        got_d = [permute(c, to_x) for c in cuts]
        side = [permute(w, to_core) for w in (wg, wu, wd)]
        w13, w2 = call(own_kernel, (shape(slots, D, 2 * F), shape(slots, F, D)),
                       [smem] + [hbm] * 6, ring(F, TILE) + ring(D, TILE // 4), 6 * block)(place, wg, wu, wd, *side)

        def later(kernel, dest, got, out, cols, tile, rel_in=hbm):
            rel = permute(got, to_relay)
            return call(functools.partial(kernel, dest), shape(*out.shape), [smem, hbm, rel_in, hbm],
                        ring(cols, tile), 3 * got.size * 2, {3: 0})(place, got, rel, out)

        w13 = later(both_kernel, lambda o, j: half(o, j, 0), got_g, w13, F, TILE)
        w13 = later(both_kernel, lambda o, j: half(o, j, 1), got_u, w13, F, TILE)
        w2 = later(both_kernel, lambda o, j: rows_of(o, j, 0), got_d[0], w2, D, TILE // 4)
        w2 = later(first_kernel, lambda o, j: rows_of(o, j, BOTH_ROWS), got_d[1], w2, D, TILE // 2,
                   vmem)
        r = BOTH_ROWS
        for i, got in enumerate(got_d[2:]):
            kernel, ins, scratch = ((other_kernel, [smem, hbm, hbm], ring(D, TILE // 4, 1)) if i == 0 else
                                    (last_kernel, [vmem, vmem, hbm], [pltpu.SemaphoreType.DMA((slots,))]))
            w2 = call(functools.partial(kernel, lambda o, j, r=r: rows_of(o, j, r)),
                      shape(*w2.shape), ins, scratch, 3 * got.size * 2, {2: 0})(place, got, w2)
            r += got.shape[0]
        return w13[None], w2[None]

    spec_in = P(None, "ep", None, None)
    spec_out = P(None, ("dp", "ep"), None, None)
    return jax.shard_map(hand_over, mesh=mesh,
                         in_specs=(spec_in, spec_in, spec_in, P(None, None)),
                         out_specs=(spec_out, spec_out), check_vma=False)
```

```python
import functools

import jax
import jax.numpy as jnp
from jax import lax
from jax.experimental import pallas as pl
from jax.experimental.pallas import tpu as pltpu
from jax.sharding import PartitionSpec as P


TILE = 512
NBUF = 4
VMEM_LIMIT = 36 * 1024 * 1024
VMEM_LIMIT_WIDE = 44 * 1024 * 1024
BOTH_ROWS = 768
LAST_ROWS = (656, 96, 16)


def _shard(dp, ep, slots, a, g, j):
    return (2 * a - g) % ep if j < ((a + 1) * slots) // dp else (g + j + 1) % ep


def _devices(dp, ep, slots, flip):
    return [[a * ep + g for a in range(dp) for g in range(ep) if _shard(dp, ep, slots, a, g, j) == g ^ flip]
            for j in range(slots)]


def _any(me, devices):
    hit = me < 0
    for n in sorted(set(devices)):
        hit = jnp.logical_or(hit, me == n)
    return hit


def _tiles(rows, tile):
    out, r = [], 0
    for n in [tile // 8, tile // 4, tile - tile // 8 - tile // 4] + [tile] * rows:
        n = min(n, rows - r)
        if n:
            out.append((r, n))
        r += n
    return out


def _stream(steps, read, writes):
    for t in range(min(NBUF, steps)):
        read(t).start()
    for t in range(steps):
        read(t).wait()
        writes(t, lambda c: c.start())
        writes(t, lambda c: c.wait())
        if t + NBUF < steps:
            read(t + NBUF).start()


def _both(src, dests, experts, who, me, buf, rsem, wsem):
    tiles = _tiles(src.shape[1], buf.shape[2])

    def read(t):
        r, n = tiles[t]
        return pltpu.make_async_copy(src.at[:, pl.ds(r, n)], buf.at[t % NBUF, :, pl.ds(0, n)], rsem.at[t % NBUF])

    def writes(t, act):
        r, n = tiles[t]
        for j, dest in enumerate(dests):
            if who[j]:
                @pl.when(_any(me, who[j]))
                def _():
                    act(pltpu.make_async_copy(buf.at[t % NBUF, experts[j], pl.ds(0, n)], dest(r, n),
                                              wsem.at[t % NBUF, j]))

    _stream(len(tiles), read, writes)


def _one(src, dests, wanted, buf, rsem, wsem):
    tiles = _tiles(src.shape[0], buf.shape[2])

    def read(t):
        r, n = tiles[t]
        return pltpu.make_async_copy(src.at[pl.ds(r, n)], buf.at[t % NBUF, 0, pl.ds(0, n)], rsem.at[t % NBUF])

    def writes(t, act):
        r, n = tiles[t]
        for j, dest in enumerate(dests):
            def go():
                act(pltpu.make_async_copy(buf.at[t % NBUF, 0, pl.ds(0, n)], dest(r, n), wsem.at[t % NBUF, j]))

            if wanted[j] is True:
                go()
            elif wanted[j] is not None:
                pl.when(wanted[j])(go)

    _stream(len(tiles), read, writes)


def solution(mesh):
    dp = mesh.shape["dp"]
    ep = mesh.shape["ep"]
    axes = ("dp", "ep")
    hbm = pl.BlockSpec(memory_space=pltpu.HBM)
    vmem = pl.BlockSpec(memory_space=pltpu.VMEM)
    smem = pl.BlockSpec(memory_space=pltpu.SMEM)

    def hand_over(w_gate, w_up, w_down, place):
        wg, wu, wd = w_gate[0], w_up[0], w_down[0]
        n_exp, D, F = wg.shape
        slots = place.shape[1] // (dp * ep)
        own, across, beside, relayed = (_devices(dp, ep, slots, f) for f in (0, 2, 1, 3))
        to_x = [(n ^ 2, n) for n in sorted(set(sum(across, [])) | {m ^ 1 for m in sum(relayed, [])})]
        to_core = [(n ^ 1, n) for n in sorted(set(sum(beside, [])))]
        to_relay = [(n ^ 1, n) for n in sorted(set(sum(relayed, [])))]

        def ring(cols, tile, experts=n_exp):
            return [pltpu.VMEM((NBUF, experts, tile, cols), jnp.bfloat16),
                    pltpu.SemaphoreType.DMA((NBUF,)), pltpu.SemaphoreType.DMA((NBUF, slots))]

        def where():
            return lax.axis_index("dp") * ep + lax.axis_index("ep")

        def half(out, j, k):
            return lambda r, n: out.at[j, pl.ds(r, n), pl.ds(k * F, F)]

        def rows_of(out, j, first):
            return lambda r, n: out.at[j, pl.ds(first + r, n)]

        def picks(place_ref, me):
            return [lax.rem(place_ref[0, me * slots + j], n_exp) for j in range(slots)]

        def early(pick, me, flip):
            e = me * 0
            for _, n in to_x:
                on = [j for j in range(slots) if n ^ 1 in relayed[j]]
                here = [j for j in range(slots) if n in across[j]]
                if on:
                    first = pick(n ^ 1, on[0])
                else:
                    first = jnp.where(2 * sum(pick(n, j) for j in here) > len(here), 1, 0)
                e = jnp.where(me == n ^ flip, first, e)
            return e

        def scalars(place_ref):
            return lambda n, j: lax.rem(place_ref[0, n * slots + j], n_exp)

        def bits(place_ref):
            lane = lax.broadcasted_iota(jnp.int32, place_ref.shape, 1)
            mask = jnp.sum(jnp.left_shift(jnp.bitwise_and(place_ref[...], 1), lane))
            return lambda n, j: jnp.bitwise_and(jnp.right_shift(mask, n * slots + j), 1)

        def call(kernel, out_shape, in_specs, scratch, size, aliases=None, cols=0):
            return pl.pallas_call(
                kernel, out_shape=out_shape, in_specs=in_specs,
                out_specs=jax.tree.map(lambda _: hbm, out_shape), scratch_shapes=scratch,
                input_output_aliases=aliases or {},
                compiler_params=pltpu.CompilerParams(vmem_limit_bytes=VMEM_LIMIT_WIDE if cols == F else VMEM_LIMIT),
                cost_estimate=pl.CostEstimate(flops=0, bytes_accessed=size, transcendentals=0))

        def own_kernel(place_ref, g, u, d, cg, cu, cd, o13, o2, buf_f, rf, wf, buf_d, rd, wd_):
            me = where()
            e = picks(place_ref, me)

            many = [n for n in range(dp * ep) if sum(n in d for d in own) > 1]

            @pl.when(_any(me, many))
            def _():
                _both(g, [half(o13, j, 0) for j in range(slots)], e, own, me, buf_f, rf, wf)
                _both(u, [half(o13, j, 1) for j in range(slots)], e, own, me, buf_f, rf, wf)
                _both(d, [rows_of(o2, j, 0) for j in range(slots)], e, own, me, buf_d, rd, wd_)

            for who, blocks in ((own, (g, u, d)), (beside, (cg, cu, cd))):
                for j in range(slots):
                    single = [n for n in who[j] if who is beside or n not in many]
                    if single:
                        @pl.when(_any(me, single))
                        def _():
                            _one(blocks[0].at[e[j]], [half(o13, j, 0)], [True], buf_f, rf, wf)
                            _one(blocks[1].at[e[j]], [half(o13, j, 1)], [True], buf_f, rf, wf)
                            _one(blocks[2].at[e[j]], [rows_of(o2, j, 0)], [True], buf_d, rd, wd_)

        def both_kernel(dest, place_ref, got, rel, _, out, buf, rs, ws):
            me = where()
            e = picks(place_ref, me)

            @pl.when(_any(me, sum(across, [])))
            def _():
                _both(got, [dest(out, j) for j in range(slots)], e, across, me, buf, rs, ws)

            for j in range(slots):
                if relayed[j]:
                    @pl.when(_any(me, relayed[j]))
                    def _():
                        _one(rel.at[e[j]], [dest(out, j)], [True], buf, rs, ws)

        def wants(pick, me, first):
            a = early(pick, me, 0)
            return [jnp.logical_and(_any(me, across[j]), (pick(me, j) == a) == first) if across[j] else None
                    for j in range(slots)]

        def first_kernel(dest, place_ref, got, rel, _, out, buf, rs, ws):
            me = where()

            @pl.when(_any(me, sum(across, [])))
            def _():
                _one(got, [dest(out, j) for j in range(slots)], wants(scalars(place_ref), me, True), buf, rs, ws)

            for j in range(slots):
                if relayed[j]:
                    @pl.when(_any(me, relayed[j]))
                    def _():
                        copy = pltpu.make_async_copy(rel, dest(out, j)(0, rel.shape[0]), rs.at[0])
                        copy.start()
                        copy.wait()

        def last_kernel(dest, place_ref, got, _, out, ws):
            want = wants(bits(place_ref), where(), False)
            for act in (lambda c: c.start(), lambda c: c.wait()):
                for j in range(slots):
                    if want[j] is not None:
                        @pl.when(want[j])
                        def _():
                            act(pltpu.make_async_copy(got, dest(out, j)(0, got.shape[0]), ws.at[j]))

        def cut_kernel(place_ref, d, both, *rest):
            pieces, (buf, rs, ws) = rest[:-3], rest[-3:]
            e = early(scalars(place_ref), where(), 2)
            tile = buf.shape[2]
            steps = [(d.at[x, pl.ds(r, n)], both.at[x, pl.ds(r, n)], n)
                     for x in range(n_exp) for r, n in _tiles(BOTH_ROWS, tile)]
            first = BOTH_ROWS
            for i, o in enumerate(pieces):
                x = e if i == 0 else 1 - e
                for r, n in _tiles(o.shape[0], tile):
                    steps.append((d.at[x, pl.ds(first + r, n)], o.at[pl.ds(r, n)], n))
                first = BOTH_ROWS if i == 0 else first + o.shape[0]

            def read(t):
                src, _, n = steps[t]
                return pltpu.make_async_copy(src, buf.at[t % NBUF, 0, pl.ds(0, n)], rs.at[t % NBUF])

            def writes(t, act):
                _, dst, n = steps[t]
                act(pltpu.make_async_copy(buf.at[t % NBUF, 0, pl.ds(0, n)], dst, ws.at[t % NBUF, 0]))

            _stream(len(steps), read, writes)

        def permute(x, pairs):
            return lax.ppermute(x, axes, pairs)

        def shape(*dims):
            return jax.ShapeDtypeStruct(dims, jnp.bfloat16)

        block = wg.size * wg.dtype.itemsize
        got_g = permute(wg, to_x)
        got_u = permute(wu, to_x)
        cuts = call(cut_kernel,
                    [shape(n_exp, BOTH_ROWS, D), shape(F - BOTH_ROWS, D)] + [shape(n, D) for n in LAST_ROWS],
                    [smem, hbm], ring(D, TILE // 2, 1), 2 * block)(place, wd)
        got_d = [permute(c, to_x) for c in cuts]
        side = [permute(w, to_core) for w in (wg, wu, wd)]
        w13, w2 = call(own_kernel, (shape(slots, D, 2 * F), shape(slots, F, D)),
                       [smem] + [hbm] * 6, ring(F, TILE) + ring(D, TILE // 4), 6 * block)(place, wg, wu, wd, *side)

        def later(kernel, dest, got, out, cols, tile, rel_in=hbm):
            rel = permute(got, to_relay)
            return call(functools.partial(kernel, dest), shape(*out.shape), [smem, hbm, rel_in, hbm],
                        ring(cols, tile), 3 * got.size * 2, {3: 0}, cols)(place, got, rel, out)

        w13 = later(both_kernel, lambda o, j: half(o, j, 0), got_g, w13, F, TILE)
        w13 = later(both_kernel, lambda o, j: half(o, j, 1), got_u, w13, F, TILE)
        w2 = later(both_kernel, lambda o, j: rows_of(o, j, 0), got_d[0], w2, D, TILE // 4)
        w2 = later(first_kernel, lambda o, j: rows_of(o, j, BOTH_ROWS), got_d[1], w2, D, TILE // 2,
                   vmem)
        r = BOTH_ROWS
        for got in got_d[2:]:
            w2 = call(functools.partial(last_kernel, lambda o, j, r=r: rows_of(o, j, r)),
                      shape(*w2.shape), [vmem, vmem, hbm], [pltpu.SemaphoreType.DMA((slots,))],
                      3 * got.size * 2, {2: 0})(place, got, w2)
            r += got.shape[0]
        return w13[None], w2[None]

    spec_in = P(None, "ep", None, None)
    spec_out = P(None, ("dp", "ep"), None, None)
    return jax.shard_map(hand_over, mesh=mesh,
                         in_specs=(spec_in, spec_in, spec_in, P(None, None)),
                         out_specs=(spec_out, spec_out), check_vma=False)
```

```python
import functools

import jax
import jax.numpy as jnp
from jax import lax
from jax.experimental import pallas as pl
from jax.experimental.pallas import tpu as pltpu
from jax.sharding import PartitionSpec as P


TILE = 512
NBUF = 4
VMEM_LIMIT = 36 * 1024 * 1024
VMEM_LIMIT_WIDE = 44 * 1024 * 1024
BOTH_ROWS = 960
LAST_ROWS = (464, 96, 16)


def _shard(dp, ep, slots, a, g, j):
    return (2 * a - g) % ep if j < ((a + 1) * slots) // dp else (g + j + 1) % ep


def _devices(dp, ep, slots, flip):
    return [[a * ep + g for a in range(dp) for g in range(ep) if _shard(dp, ep, slots, a, g, j) == g ^ flip]
            for j in range(slots)]


def _any(me, devices):
    hit = me < 0
    for n in sorted(set(devices)):
        hit = jnp.logical_or(hit, me == n)
    return hit


def _tiles(rows, tile):
    out, r = [], 0
    for n in [tile // 8, tile // 4, tile - tile // 8 - tile // 4] + [tile] * rows:
        n = min(n, rows - r)
        if n:
            out.append((r, n))
        r += n
    return out


def _stream(steps, read, writes):
    for t in range(min(NBUF, steps)):
        read(t).start()
    for t in range(steps):
        read(t).wait()
        writes(t, lambda c: c.start())
        writes(t, lambda c: c.wait())
        if t + NBUF < steps:
            read(t + NBUF).start()


def _both(src, dests, experts, who, me, buf, rsem, wsem):
    tiles = _tiles(src.shape[1], buf.shape[2])

    def read(t):
        r, n = tiles[t]
        return pltpu.make_async_copy(src.at[:, pl.ds(r, n)], buf.at[t % NBUF, :, pl.ds(0, n)], rsem.at[t % NBUF])

    def writes(t, act):
        r, n = tiles[t]
        for j, dest in enumerate(dests):
            if who[j]:
                @pl.when(_any(me, who[j]))
                def _():
                    act(pltpu.make_async_copy(buf.at[t % NBUF, experts[j], pl.ds(0, n)], dest(r, n),
                                              wsem.at[t % NBUF, j]))

    _stream(len(tiles), read, writes)


def _one(src, dests, wanted, buf, rsem, wsem):
    tiles = _tiles(src.shape[0], buf.shape[2])

    def read(t):
        r, n = tiles[t]
        return pltpu.make_async_copy(src.at[pl.ds(r, n)], buf.at[t % NBUF, 0, pl.ds(0, n)], rsem.at[t % NBUF])

    def writes(t, act):
        r, n = tiles[t]
        for j, dest in enumerate(dests):
            def go():
                act(pltpu.make_async_copy(buf.at[t % NBUF, 0, pl.ds(0, n)], dest(r, n), wsem.at[t % NBUF, j]))

            if wanted[j] is True:
                go()
            elif wanted[j] is not None:
                pl.when(wanted[j])(go)

    _stream(len(tiles), read, writes)


def solution(mesh):
    dp = mesh.shape["dp"]
    ep = mesh.shape["ep"]
    axes = ("dp", "ep")
    hbm = pl.BlockSpec(memory_space=pltpu.HBM)
    vmem = pl.BlockSpec(memory_space=pltpu.VMEM)
    smem = pl.BlockSpec(memory_space=pltpu.SMEM)

    def hand_over(w_gate, w_up, w_down, place):
        wg, wu, wd = w_gate[0], w_up[0], w_down[0]
        n_exp, D, F = wg.shape
        slots = place.shape[1] // (dp * ep)
        own, across, beside, relayed = (_devices(dp, ep, slots, f) for f in (0, 2, 1, 3))
        to_x = [(n ^ 2, n) for n in sorted(set(sum(across, [])) | {m ^ 1 for m in sum(relayed, [])})]
        to_core = [(n ^ 1, n) for n in sorted(set(sum(beside, [])))]
        to_relay = [(n ^ 1, n) for n in sorted(set(sum(relayed, [])))]
        last_from = {n: n ^ 2 | 1 for _, n in to_x}
        lent = [(n ^ 2, m) for n, m in last_from.items() if m != n ^ 2]
        to_last = [(m, n) for n, m in last_from.items()]

        def ring(cols, tile, experts=n_exp):
            return [pltpu.VMEM((NBUF, experts, tile, cols), jnp.bfloat16),
                    pltpu.SemaphoreType.DMA((NBUF,)), pltpu.SemaphoreType.DMA((NBUF, slots))]

        def where():
            return lax.axis_index("dp") * ep + lax.axis_index("ep")

        def half(out, j, k):
            return lambda r, n: out.at[j, pl.ds(r, n), pl.ds(k * F, F)]

        def rows_of(out, j, first):
            return lambda r, n: out.at[j, pl.ds(first + r, n)]

        def picks(place_ref, me):
            return [lax.rem(place_ref[0, me * slots + j], n_exp) for j in range(slots)]

        def early(pick, me, actor):
            e = me * 0
            for _, n in to_x:
                on = [j for j in range(slots) if n ^ 1 in relayed[j]]
                here = [j for j in range(slots) if n in across[j]]
                if on:
                    first = pick(n ^ 1, on[0])
                else:
                    first = jnp.where(2 * sum(pick(n, j) for j in here) > len(here), 1, 0)
                e = jnp.where(me == actor(n), first, e)
            return e

        def scalars(place_ref):
            return lambda n, j: lax.rem(place_ref[0, n * slots + j], n_exp)

        def bits(place_ref):
            lane = lax.broadcasted_iota(jnp.int32, place_ref.shape, 1)
            mask = jnp.sum(jnp.left_shift(jnp.bitwise_and(place_ref[...], 1), lane))
            return lambda n, j: jnp.bitwise_and(jnp.right_shift(mask, n * slots + j), 1)

        def call(kernel, out_shape, in_specs, scratch, size, aliases=None, cols=0):
            return pl.pallas_call(
                kernel, out_shape=out_shape, in_specs=in_specs,
                out_specs=jax.tree.map(lambda _: hbm, out_shape), scratch_shapes=scratch,
                input_output_aliases=aliases or {},
                compiler_params=pltpu.CompilerParams(vmem_limit_bytes=VMEM_LIMIT_WIDE if cols == F else VMEM_LIMIT),
                cost_estimate=pl.CostEstimate(flops=0, bytes_accessed=size, transcendentals=0))

        def own_kernel(place_ref, g, u, d, cg, cu, cd, o13, o2, buf_f, rf, wf, buf_d, rd, wd_):
            me = where()
            e = picks(place_ref, me)

            many = [n for n in range(dp * ep) if sum(n in d for d in own) > 1]

            @pl.when(_any(me, many))
            def _():
                _both(g, [half(o13, j, 0) for j in range(slots)], e, own, me, buf_f, rf, wf)
                _both(u, [half(o13, j, 1) for j in range(slots)], e, own, me, buf_f, rf, wf)
                _both(d, [rows_of(o2, j, 0) for j in range(slots)], e, own, me, buf_d, rd, wd_)

            for who, blocks in ((own, (g, u, d)), (beside, (cg, cu, cd))):
                for j in range(slots):
                    single = [n for n in who[j] if who is beside or n not in many]
                    if single:
                        @pl.when(_any(me, single))
                        def _():
                            _one(blocks[0].at[e[j]], [half(o13, j, 0)], [True], buf_f, rf, wf)
                            _one(blocks[1].at[e[j]], [half(o13, j, 1)], [True], buf_f, rf, wf)
                            _one(blocks[2].at[e[j]], [rows_of(o2, j, 0)], [True], buf_d, rd, wd_)

        def both_kernel(dest, place_ref, got, rel, _, out, buf, rs, ws):
            me = where()
            e = picks(place_ref, me)

            @pl.when(_any(me, sum(across, [])))
            def _():
                _both(got, [dest(out, j) for j in range(slots)], e, across, me, buf, rs, ws)

            for j in range(slots):
                if relayed[j]:
                    @pl.when(_any(me, relayed[j]))
                    def _():
                        _one(rel.at[e[j]], [dest(out, j)], [True], buf, rs, ws)

        def wants(pick, me, first):
            a = early(pick, me, lambda n: n)
            return [jnp.logical_and(_any(me, across[j]), (pick(me, j) == a) == first) if across[j] else None
                    for j in range(slots)]

        def first_kernel(dest, place_ref, got, rel, _, out, buf, rs, ws):
            me = where()

            @pl.when(_any(me, sum(across, [])))
            def _():
                _one(got, [dest(out, j) for j in range(slots)], wants(scalars(place_ref), me, True), buf, rs, ws)

            for j in range(slots):
                if relayed[j]:
                    @pl.when(_any(me, relayed[j]))
                    def _():
                        copy = pltpu.make_async_copy(rel, dest(out, j)(0, rel.shape[0]), rs.at[0])
                        copy.start()
                        copy.wait()

        def last_kernel(dest, place_ref, got, _, out, ws):
            want = wants(bits(place_ref), where(), False)
            for act in (lambda c: c.start(), lambda c: c.wait()):
                for j in range(slots):
                    if want[j] is not None:
                        @pl.when(want[j])
                        def _():
                            act(pltpu.make_async_copy(got, dest(out, j)(0, got.shape[0]), ws.at[j]))

        def cut(pieces, buf, rs, ws):
            steps = []
            for src, dst in pieces:
                steps += [(src.at[pl.ds(r, n)], dst.at[pl.ds(r, n)], n) for r, n in _tiles(dst.shape[0], buf.shape[2])]

            def read(t):
                src, _, n = steps[t]
                return pltpu.make_async_copy(src, buf.at[t % NBUF, 0, pl.ds(0, n)], rs.at[t % NBUF])

            def writes(t, act):
                _, dst, n = steps[t]
                act(pltpu.make_async_copy(buf.at[t % NBUF, 0, pl.ds(0, n)], dst, ws.at[t % NBUF, 0]))

            _stream(len(steps), read, writes)

        def cut_kernel(place_ref, d, both, first, buf, rs, ws):
            e = early(scalars(place_ref), where(), lambda n: n ^ 2)
            cut([(d.at[x, pl.ds(0, BOTH_ROWS)], both.at[x]) for x in range(n_exp)]
                + [(d.at[e, pl.ds(BOTH_ROWS, F - BOTH_ROWS)], first)], buf, rs, ws)

        def cut_last_kernel(place_ref, d, cd, *rest):
            outs, (buf, rs, ws) = rest[:-3], rest[-3:]
            me = where()
            x = 1 - early(scalars(place_ref), me, lambda n: last_from[n])
            for src, mine in ((d, [m for m, n in to_last if m == n ^ 2]), (cd, [m for _, m in lent])):
                @pl.when(_any(me, mine))
                def _():
                    pieces, r = [], BOTH_ROWS
                    for o in outs:
                        pieces.append((src.at[x, pl.ds(r, o.shape[0])], o))
                        r += o.shape[0]
                    cut(pieces, buf, rs, ws)

        def permute(x, pairs):
            return lax.ppermute(x, axes, pairs)

        def shape(*dims):
            return jax.ShapeDtypeStruct(dims, jnp.bfloat16)

        block = wg.size * wg.dtype.itemsize
        got_g = permute(wg, to_x)
        got_u = permute(wu, to_x)
        cuts = call(cut_kernel, [shape(n_exp, BOTH_ROWS, D), shape(F - BOTH_ROWS, D)],
                    [smem, hbm], ring(D, TILE // 2, 1), 2 * block)(place, wd)
        side = [permute(w, to_core + (lent if i == 2 else [])) for i, w in enumerate((wg, wu, wd))]
        lasts = call(cut_last_kernel, [shape(n, D) for n in LAST_ROWS],
                     [smem, hbm, hbm], ring(D, TILE // 2, 1), 2 * block)(place, wd, side[2])
        got_d = [permute(c, to_x if i < 2 else to_last) for i, c in enumerate(cuts + lasts)]
        w13, w2 = call(own_kernel, (shape(slots, D, 2 * F), shape(slots, F, D)),
                       [smem] + [hbm] * 6, ring(F, TILE) + ring(D, TILE // 4), 6 * block)(place, wg, wu, wd, *side)

        def later(kernel, dest, got, out, cols, tile, rel_in=hbm):
            rel = permute(got, to_relay)
            return call(functools.partial(kernel, dest), shape(*out.shape), [smem, hbm, rel_in, hbm],
                        ring(cols, tile), 3 * got.size * 2, {3: 0}, cols)(place, got, rel, out)

        w13 = later(both_kernel, lambda o, j: half(o, j, 0), got_g, w13, F, TILE)
        w13 = later(both_kernel, lambda o, j: half(o, j, 1), got_u, w13, F, TILE)
        w2 = later(both_kernel, lambda o, j: rows_of(o, j, 0), got_d[0], w2, D, TILE // 4)
        w2 = later(first_kernel, lambda o, j: rows_of(o, j, BOTH_ROWS), got_d[1], w2, D, TILE // 2,
                   vmem)
        r = BOTH_ROWS
        for got in got_d[2:]:
            w2 = call(functools.partial(last_kernel, lambda o, j, r=r: rows_of(o, j, r)),
                      shape(*w2.shape), [vmem, vmem, hbm], [pltpu.SemaphoreType.DMA((slots,))],
                      3 * got.size * 2, {2: 0})(place, got, w2)
            r += got.shape[0]
        return w13[None], w2[None]

    spec_in = P(None, "ep", None, None)
    spec_out = P(None, ("dp", "ep"), None, None)
    return jax.shard_map(hand_over, mesh=mesh,
                         in_specs=(spec_in, spec_in, spec_in, P(None, None)),
                         out_specs=(spec_out, spec_out), check_vma=False)
```

```python
import functools

import jax
import jax.numpy as jnp
from jax import lax
from jax.experimental import pallas as pl
from jax.experimental.pallas import tpu as pltpu
from jax.sharding import PartitionSpec as P


TILE = 512
NBUF = 4
VMEM_LIMIT = 36 * 1024 * 1024
VMEM_LIMIT_WIDE = 44 * 1024 * 1024
BOTH_ROWS = 768
LAST = ((1504, 1536, 0, 512, True), (768, 1424, 0, 4096, False), (1424, 1504, 0, 4096, False), (1504, 1536, 512, 4096, False))


def _shard(dp, ep, slots, a, g, j):
    return (2 * a - g) % ep if j < ((a + 1) * slots) // dp else (g + j + 1) % ep


def _devices(dp, ep, slots, flip):
    return [[a * ep + g for a in range(dp) for g in range(ep) if _shard(dp, ep, slots, a, g, j) == g ^ flip]
            for j in range(slots)]


def _any(me, devices):
    hit = me < 0
    for n in sorted(set(devices)):
        hit = jnp.logical_or(hit, me == n)
    return hit


def _tiles(rows, tile):
    out, r = [], 0
    for n in [tile // 8, tile // 4, tile - tile // 8 - tile // 4] + [tile] * rows:
        n = min(n, rows - r)
        if n:
            out.append((r, n))
        r += n
    return out


def _stream(steps, read, writes):
    for t in range(min(NBUF, steps)):
        read(t).start()
    for t in range(steps):
        read(t).wait()
        writes(t, lambda c: c.start())
        writes(t, lambda c: c.wait())
        if t + NBUF < steps:
            read(t + NBUF).start()


def _both(src, dests, experts, who, me, buf, rsem, wsem):
    tiles = _tiles(src.shape[1], buf.shape[2])

    def read(t):
        r, n = tiles[t]
        return pltpu.make_async_copy(src.at[:, pl.ds(r, n)], buf.at[t % NBUF, :, pl.ds(0, n)], rsem.at[t % NBUF])

    def writes(t, act):
        r, n = tiles[t]
        for j, dest in enumerate(dests):
            if who[j]:
                @pl.when(_any(me, who[j]))
                def _():
                    act(pltpu.make_async_copy(buf.at[t % NBUF, experts[j], pl.ds(0, n)], dest(r, n),
                                              wsem.at[t % NBUF, j]))

    _stream(len(tiles), read, writes)


def _one(src, dests, wanted, buf, rsem, wsem):
    tiles = _tiles(src.shape[0], buf.shape[2])

    def read(t):
        r, n = tiles[t]
        return pltpu.make_async_copy(src.at[pl.ds(r, n)], buf.at[t % NBUF, 0, pl.ds(0, n)], rsem.at[t % NBUF])

    def writes(t, act):
        r, n = tiles[t]
        for j, dest in enumerate(dests):
            def go():
                act(pltpu.make_async_copy(buf.at[t % NBUF, 0, pl.ds(0, n)], dest(r, n), wsem.at[t % NBUF, j]))

            if wanted[j] is True:
                go()
            elif wanted[j] is not None:
                pl.when(wanted[j])(go)

    _stream(len(tiles), read, writes)


def solution(mesh):
    dp = mesh.shape["dp"]
    ep = mesh.shape["ep"]
    axes = ("dp", "ep")
    hbm = pl.BlockSpec(memory_space=pltpu.HBM)
    vmem = pl.BlockSpec(memory_space=pltpu.VMEM)
    smem = pl.BlockSpec(memory_space=pltpu.SMEM)

    def hand_over(w_gate, w_up, w_down, place):
        wg, wu, wd = w_gate[0], w_up[0], w_down[0]
        n_exp, D, F = wg.shape
        slots = place.shape[1] // (dp * ep)
        own, across, beside, relayed = (_devices(dp, ep, slots, f) for f in (0, 2, 1, 3))
        to_x = [(n ^ 2, n) for n in sorted(set(sum(across, [])) | {m ^ 1 for m in sum(relayed, [])})]
        to_core = [(n ^ 1, n) for n in sorted(set(sum(beside, [])))]
        to_relay = [(n ^ 1, n) for n in sorted(set(sum(relayed, [])))]
        to_block = [(m if n ^ 1 in sum(relayed, []) else m ^ ep, n) for m, n in to_x]

        def ring(cols, tile, experts=n_exp):
            return [pltpu.VMEM((NBUF, experts, tile, cols), jnp.bfloat16),
                    pltpu.SemaphoreType.DMA((NBUF,)), pltpu.SemaphoreType.DMA((NBUF, slots))]

        def where():
            return lax.axis_index("dp") * ep + lax.axis_index("ep")

        def half(out, j, k):
            return lambda r, n: out.at[j, pl.ds(r, n), pl.ds(k * F, F)]

        def rows_of(out, j, first):
            return lambda r, n: out.at[j, pl.ds(first + r, n)]

        def picks(place_ref, me):
            return [lax.rem(place_ref[0, me * slots + j], n_exp) for j in range(slots)]

        def early(pick, me, actors):
            e = me * 0
            for _, n in to_x:
                on = [j for j in range(slots) if n ^ 1 in relayed[j]]
                here = [j for j in range(slots) if n in across[j]]
                if on:
                    first = pick(n ^ 1, on[0])
                else:
                    first = jnp.where(2 * sum(pick(n, j) for j in here) > len(here), 1, 0)
                e = jnp.where(_any(me, actors(n)), first, e)
            return e

        def scalars(place_ref):
            return lambda n, j: lax.rem(place_ref[0, n * slots + j], n_exp)

        def bits(place_ref):
            lane = lax.broadcasted_iota(jnp.int32, place_ref.shape, 1)
            mask = jnp.sum(jnp.left_shift(jnp.bitwise_and(place_ref[...], 1), lane))
            return lambda n, j: jnp.bitwise_and(jnp.right_shift(mask, n * slots + j), 1)

        def call(kernel, out_shape, in_specs, scratch, size, aliases=None, cols=0):
            return pl.pallas_call(
                kernel, out_shape=out_shape, in_specs=in_specs,
                out_specs=jax.tree.map(lambda _: hbm, out_shape), scratch_shapes=scratch,
                input_output_aliases=aliases or {},
                compiler_params=pltpu.CompilerParams(vmem_limit_bytes=VMEM_LIMIT_WIDE if cols == F else VMEM_LIMIT),
                cost_estimate=pl.CostEstimate(flops=0, bytes_accessed=size, transcendentals=0))

        def own_kernel(place_ref, g, u, d, cg, cu, cd, o13, o2, buf_f, rf, wf, buf_d, rd, wd_):
            me = where()
            e = picks(place_ref, me)

            many = [n for n in range(dp * ep) if sum(n in d for d in own) > 1]

            @pl.when(_any(me, many))
            def _():
                _both(g, [half(o13, j, 0) for j in range(slots)], e, own, me, buf_f, rf, wf)
                _both(u, [half(o13, j, 1) for j in range(slots)], e, own, me, buf_f, rf, wf)
                _both(d, [rows_of(o2, j, 0) for j in range(slots)], e, own, me, buf_d, rd, wd_)

            for who, blocks in ((own, (g, u, d)), (beside, (cg, cu, cd))):
                for j in range(slots):
                    single = [n for n in who[j] if who is beside or n not in many]
                    if single:
                        @pl.when(_any(me, single))
                        def _():
                            _one(blocks[0].at[e[j]], [half(o13, j, 0)], [True], buf_f, rf, wf)
                            _one(blocks[1].at[e[j]], [half(o13, j, 1)], [True], buf_f, rf, wf)
                            _one(blocks[2].at[e[j]], [rows_of(o2, j, 0)], [True], buf_d, rd, wd_)

        def both_kernel(dest, place_ref, got, rel, _, out, buf, rs, ws):
            me = where()
            e = picks(place_ref, me)

            @pl.when(_any(me, sum(across, [])))
            def _():
                _both(got, [dest(out, j) for j in range(slots)], e, across, me, buf, rs, ws)

            for j in range(slots):
                if relayed[j]:
                    @pl.when(_any(me, relayed[j]))
                    def _():
                        _one(rel.at[e[j]], [dest(out, j)], [True], buf, rs, ws)

        def wants(pick, me, first):
            a = early(pick, me, lambda n: [n])
            return [jnp.logical_and(_any(me, across[j]), (pick(me, j) == a) == first) if across[j] else None
                    for j in range(slots)]

        def first_kernel(dest, place_ref, got, rel, _, out, buf, rs, ws):
            me = where()

            @pl.when(_any(me, sum(across, [])))
            def _():
                _one(got, [dest(out, j) for j in range(slots)], wants(scalars(place_ref), me, True), buf, rs, ws)

            for j in range(slots):
                if relayed[j]:
                    @pl.when(_any(me, relayed[j]))
                    def _():
                        copy = pltpu.make_async_copy(rel, dest(out, j)(0, rel.shape[0]), rs.at[0])
                        copy.start()
                        copy.wait()

        def last_kernel(dest, place_ref, got, _, out, ws):
            want = wants(bits(place_ref), where(), False)
            for act in (lambda c: c.start(), lambda c: c.wait()):
                for j in range(slots):
                    if want[j] is not None:
                        @pl.when(want[j])
                        def _():
                            act(pltpu.make_async_copy(got, dest(out, j), ws.at[j]))

        def cut_kernel(place_ref, d, both, *rest):
            pieces, (buf, rs, ws) = rest[:-3], rest[-3:]
            e = early(scalars(place_ref), where(), lambda n: [m for m, r in to_x + to_block if r == n])
            tile = buf.shape[2]
            steps = [(d.at[x, pl.ds(r, n)], both.at[x, pl.ds(r, n)], n)
                     for x in range(n_exp) for r, n in _tiles(BOTH_ROWS, tile)]
            rects = [(e, BOTH_ROWS, F, 0, D)] + [(1 - e, r0, r1, c0, c1) for r0, r1, c0, c1, _ in LAST]
            for (x, r0, r1, c0, c1), o in zip(rects, pieces):
                for r, n in _tiles(r1 - r0, tile):
                    steps.append((d.at[x, pl.ds(r0 + r, n), pl.ds(c0, c1 - c0)], o.at[pl.ds(r, n)], n))

            def part(t):
                return buf.at[t % NBUF, 0, pl.ds(0, steps[t][2]), pl.ds(0, steps[t][0].shape[1])]

            def read(t):
                return pltpu.make_async_copy(steps[t][0], part(t), rs.at[t % NBUF])

            def writes(t, act):
                act(pltpu.make_async_copy(part(t), steps[t][1], ws.at[t % NBUF, 0]))

            _stream(len(steps), read, writes)

        def permute(x, pairs):
            return lax.ppermute(x, axes, pairs)

        def shape(*dims):
            return jax.ShapeDtypeStruct(dims, jnp.bfloat16)

        block = wg.size * wg.dtype.itemsize
        got_g = permute(wg, to_x)
        got_u = permute(wu, to_x)
        cuts = call(cut_kernel,
                    [shape(n_exp, BOTH_ROWS, D), shape(F - BOTH_ROWS, D)] + [shape(r1 - r0, c1 - c0) for r0, r1, c0, c1, _ in LAST],
                    [smem, hbm], ring(D, TILE // 2, 1), 2 * block)(place, wd)
        got_d = [permute(c, to_block if i > 1 and LAST[i - 2][4] else to_x) for i, c in enumerate(cuts)]
        side = [permute(w, to_core) for w in (wg, wu, wd)]
        w13, w2 = call(own_kernel, (shape(slots, D, 2 * F), shape(slots, F, D)),
                       [smem] + [hbm] * 6, ring(F, TILE) + ring(D, TILE // 4), 6 * block)(place, wg, wu, wd, *side)

        def later(kernel, dest, got, out, cols, tile, rel_in=hbm):
            rel = permute(got, to_relay)
            return call(functools.partial(kernel, dest), shape(*out.shape), [smem, hbm, rel_in, hbm],
                        ring(cols, tile), 3 * got.size * 2, {3: 0}, cols)(place, got, rel, out)

        w13 = later(both_kernel, lambda o, j: half(o, j, 0), got_g, w13, F, TILE)
        w13 = later(both_kernel, lambda o, j: half(o, j, 1), got_u, w13, F, TILE)
        w2 = later(both_kernel, lambda o, j: rows_of(o, j, 0), got_d[0], w2, D, TILE // 4)
        w2 = later(first_kernel, lambda o, j: rows_of(o, j, BOTH_ROWS), got_d[1], w2, D, TILE // 2,
                   vmem)
        for i, got in enumerate(got_d[2:]):
            r0, r1, c0, c1, _ = LAST[i]

            def rect(out, j, r0=r0, r1=r1, c0=c0, c1=c1):
                return out.at[j, pl.ds(r0, r1 - r0), pl.ds(c0, c1 - c0)]

            w2 = call(functools.partial(last_kernel, rect),
                      shape(*w2.shape), [vmem, vmem, hbm], [pltpu.SemaphoreType.DMA((slots,))],
                      3 * got.size * 2, {2: 0})(place, got, w2)
        return w13[None], w2[None]

    spec_in = P(None, "ep", None, None)
    spec_out = P(None, ("dp", "ep"), None, None)
    return jax.shard_map(hand_over, mesh=mesh,
                         in_specs=(spec_in, spec_in, spec_in, P(None, None)),
                         out_specs=(spec_out, spec_out), check_vma=False)
```

```python
import functools

import jax
import jax.numpy as jnp
from jax import lax
from jax.experimental import pallas as pl
from jax.experimental.pallas import tpu as pltpu
from jax.sharding import PartitionSpec as P


TILE = 512
NBUF = 4
VMEM_LIMIT = 36 * 1024 * 1024
VMEM_LIMIT_WIDE = 44 * 1024 * 1024
BOTH_ROWS = 768
LAST = ((1504, 1536, 0, 384, True), (768, 1424, 0, 4096, False), (1424, 1504, 0, 4096, False), (1504, 1536, 384, 4096, False))


def _shard(dp, ep, slots, a, g, j):
    return (2 * a - g) % ep if j < ((a + 1) * slots) // dp else (g + j + 1) % ep


def _devices(dp, ep, slots, flip):
    return [[a * ep + g for a in range(dp) for g in range(ep) if _shard(dp, ep, slots, a, g, j) == g ^ flip]
            for j in range(slots)]


def _any(me, devices):
    hit = me < 0
    for n in sorted(set(devices)):
        hit = jnp.logical_or(hit, me == n)
    return hit


def _tiles(rows, tile):
    out, r = [], 0
    for n in [tile // 8, tile // 4, tile - tile // 8 - tile // 4] + [tile] * rows:
        n = min(n, rows - r)
        if n:
            out.append((r, n))
        r += n
    return out


def _stream(steps, read, writes):
    for t in range(min(NBUF, steps)):
        read(t).start()
    for t in range(steps):
        read(t).wait()
        writes(t, lambda c: c.start())
        writes(t, lambda c: c.wait())
        if t + NBUF < steps:
            read(t + NBUF).start()


def _both(src, dests, experts, who, me, buf, rsem, wsem):
    tiles = _tiles(src.shape[1], buf.shape[2])

    def read(t):
        r, n = tiles[t]
        return pltpu.make_async_copy(src.at[:, pl.ds(r, n)], buf.at[t % NBUF, :, pl.ds(0, n)], rsem.at[t % NBUF])

    def writes(t, act):
        r, n = tiles[t]
        for j, dest in enumerate(dests):
            if who[j]:
                @pl.when(_any(me, who[j]))
                def _():
                    act(pltpu.make_async_copy(buf.at[t % NBUF, experts[j], pl.ds(0, n)], dest(r, n),
                                              wsem.at[t % NBUF, j]))

    _stream(len(tiles), read, writes)


def _one(src, dests, wanted, buf, rsem, wsem):
    tiles = _tiles(src.shape[0], buf.shape[2])

    def read(t):
        r, n = tiles[t]
        return pltpu.make_async_copy(src.at[pl.ds(r, n)], buf.at[t % NBUF, 0, pl.ds(0, n)], rsem.at[t % NBUF])

    def writes(t, act):
        r, n = tiles[t]
        for j, dest in enumerate(dests):
            def go():
                act(pltpu.make_async_copy(buf.at[t % NBUF, 0, pl.ds(0, n)], dest(r, n), wsem.at[t % NBUF, j]))

            if wanted[j] is True:
                go()
            elif wanted[j] is not None:
                pl.when(wanted[j])(go)

    _stream(len(tiles), read, writes)


def _flow(blocks, buf, rsem, wsem):
    steps = [(src.at[pl.ds(r, n)], dest(r, n), n) for src, dest in blocks
             for r, n in _tiles(src.shape[0], buf.shape[2])]

    def part(t):
        return buf.at[t % NBUF, 0, pl.ds(0, steps[t][2])]

    def read(t):
        return pltpu.make_async_copy(steps[t][0], part(t), rsem.at[t % NBUF])

    def writes(t, act):
        act(pltpu.make_async_copy(part(t), steps[t][1], wsem.at[t % NBUF, 0]))

    _stream(len(steps), read, writes)


def solution(mesh):
    dp = mesh.shape["dp"]
    ep = mesh.shape["ep"]
    axes = ("dp", "ep")
    hbm = pl.BlockSpec(memory_space=pltpu.HBM)
    vmem = pl.BlockSpec(memory_space=pltpu.VMEM)
    smem = pl.BlockSpec(memory_space=pltpu.SMEM)

    def hand_over(w_gate, w_up, w_down, place):
        wg, wu, wd = w_gate[0], w_up[0], w_down[0]
        n_exp, D, F = wg.shape
        slots = place.shape[1] // (dp * ep)
        own, across, beside, relayed = (_devices(dp, ep, slots, f) for f in (0, 2, 1, 3))
        to_x = [(n ^ 2, n) for n in sorted(set(sum(across, [])) | {m ^ 1 for m in sum(relayed, [])})]
        to_core = [(n ^ 1, n) for n in sorted(set(sum(beside, [])))]
        to_relay = [(n ^ 1, n) for n in sorted(set(sum(relayed, [])))]
        to_block = [(m if n ^ 1 in sum(relayed, []) else m ^ ep, n) for m, n in to_x]

        def ring(cols, tile, experts=n_exp):
            return [pltpu.VMEM((NBUF, experts, tile, cols), jnp.bfloat16),
                    pltpu.SemaphoreType.DMA((NBUF,)), pltpu.SemaphoreType.DMA((NBUF, slots))]

        def where():
            return lax.axis_index("dp") * ep + lax.axis_index("ep")

        def half(out, j, k):
            return lambda r, n: out.at[j, pl.ds(r, n), pl.ds(k * F, F)]

        def rows_of(out, j, first):
            return lambda r, n: out.at[j, pl.ds(first + r, n)]

        def picks(place_ref, me):
            return [lax.rem(place_ref[0, me * slots + j], n_exp) for j in range(slots)]

        def early(pick, me, actors):
            e = me * 0
            for _, n in to_x:
                on = [j for j in range(slots) if n ^ 1 in relayed[j]]
                here = [j for j in range(slots) if n in across[j]]
                if on:
                    first = pick(n ^ 1, on[0])
                else:
                    first = jnp.where(2 * sum(pick(n, j) for j in here) > len(here), 1, 0)
                e = jnp.where(_any(me, actors(n)), first, e)
            return e

        def scalars(place_ref):
            return lambda n, j: lax.rem(place_ref[0, n * slots + j], n_exp)

        def bits(place_ref):
            lane = lax.broadcasted_iota(jnp.int32, place_ref.shape, 1)
            mask = jnp.sum(jnp.left_shift(jnp.bitwise_and(place_ref[...], 1), lane))
            return lambda n, j: jnp.bitwise_and(jnp.right_shift(mask, n * slots + j), 1)

        def call(kernel, out_shape, in_specs, scratch, size, aliases=None, cols=0):
            return pl.pallas_call(
                kernel, out_shape=out_shape, in_specs=in_specs,
                out_specs=jax.tree.map(lambda _: hbm, out_shape), scratch_shapes=scratch,
                input_output_aliases=aliases or {},
                compiler_params=pltpu.CompilerParams(vmem_limit_bytes=VMEM_LIMIT_WIDE if cols == F else VMEM_LIMIT),
                cost_estimate=pl.CostEstimate(flops=0, bytes_accessed=size, transcendentals=0))

        def own_kernel(place_ref, g, u, d, cg, cu, cd, o13, o2, buf_f, rf, wf, buf_d, rd, wd_):
            me = where()
            e = picks(place_ref, me)

            many = [n for n in range(dp * ep) if sum(n in d for d in own) > 1]

            @pl.when(_any(me, many))
            def _():
                _both(g, [half(o13, j, 0) for j in range(slots)], e, own, me, buf_f, rf, wf)
                _both(u, [half(o13, j, 1) for j in range(slots)], e, own, me, buf_f, rf, wf)
                _both(d, [rows_of(o2, j, 0) for j in range(slots)], e, own, me, buf_d, rd, wd_)

            groups = {}
            for who, blocks in ((own, (g, u, d)), (beside, (cg, cu, cd))):
                for j in range(slots):
                    single = tuple(n for n in who[j] if who is beside or n not in many)
                    if single:
                        groups.setdefault(single, []).append((blocks, j))
            for single, items in groups.items():
                @pl.when(_any(me, single))
                def _():
                    _flow([(blocks[k].at[e[j]], half(o13, j, k)) for blocks, j in items for k in range(2)],
                          buf_f, rf, wf)
                    _flow([(blocks[2].at[e[j]], rows_of(o2, j, 0)) for blocks, j in items], buf_d, rd, wd_)

        def both_kernel(dest, place_ref, got, rel, _, out, buf, rs, ws):
            me = where()
            e = picks(place_ref, me)

            @pl.when(_any(me, sum(across, [])))
            def _():
                _both(got, [dest(out, j) for j in range(slots)], e, across, me, buf, rs, ws)

            for j in range(slots):
                if relayed[j]:
                    @pl.when(_any(me, relayed[j]))
                    def _():
                        _one(rel.at[e[j]], [dest(out, j)], [True], buf, rs, ws)

        def wants(pick, me, first):
            a = early(pick, me, lambda n: [n])
            return [jnp.logical_and(_any(me, across[j]), (pick(me, j) == a) == first) if across[j] else None
                    for j in range(slots)]

        def first_kernel(dest, place_ref, got, rel, _, out, buf, rs, ws):
            me = where()

            @pl.when(_any(me, sum(across, [])))
            def _():
                _one(got, [dest(out, j) for j in range(slots)], wants(scalars(place_ref), me, True), buf, rs, ws)

            for j in range(slots):
                if relayed[j]:
                    @pl.when(_any(me, relayed[j]))
                    def _():
                        copy = pltpu.make_async_copy(rel, dest(out, j)(0, rel.shape[0]), rs.at[0])
                        copy.start()
                        copy.wait()

        def last_kernel(dest, place_ref, got, _, out, ws):
            want = wants(bits(place_ref), where(), False)
            for act in (lambda c: c.start(), lambda c: c.wait()):
                for j in range(slots):
                    if want[j] is not None:
                        @pl.when(want[j])
                        def _():
                            act(pltpu.make_async_copy(got, dest(out, j), ws.at[j]))

        def cut_kernel(place_ref, d, both, *rest):
            pieces, (buf, rs, ws) = rest[:-3], rest[-3:]
            e = early(scalars(place_ref), where(), lambda n: [m for m, r in to_x + to_block if r == n])
            tile = buf.shape[2]
            steps = [(d.at[x, pl.ds(r, n)], both.at[x, pl.ds(r, n)], n)
                     for x in range(n_exp) for r, n in _tiles(BOTH_ROWS, tile)]
            rects = [(e, BOTH_ROWS, F, 0, D)] + [(1 - e, r0, r1, c0, c1) for r0, r1, c0, c1, _ in LAST]
            for (x, r0, r1, c0, c1), o in zip(rects, pieces):
                for r, n in _tiles(r1 - r0, tile):
                    steps.append((d.at[x, pl.ds(r0 + r, n), pl.ds(c0, c1 - c0)], o.at[pl.ds(r, n)], n))

            def part(t):
                return buf.at[t % NBUF, 0, pl.ds(0, steps[t][2]), pl.ds(0, steps[t][0].shape[1])]

            def read(t):
                return pltpu.make_async_copy(steps[t][0], part(t), rs.at[t % NBUF])

            def writes(t, act):
                act(pltpu.make_async_copy(part(t), steps[t][1], ws.at[t % NBUF, 0]))

            _stream(len(steps), read, writes)

        def permute(x, pairs):
            return lax.ppermute(x, axes, pairs)

        def shape(*dims):
            return jax.ShapeDtypeStruct(dims, jnp.bfloat16)

        block = wg.size * wg.dtype.itemsize
        got_g = permute(wg, to_x)
        got_u = permute(wu, to_x)
        cuts = call(cut_kernel,
                    [shape(n_exp, BOTH_ROWS, D), shape(F - BOTH_ROWS, D)] + [shape(r1 - r0, c1 - c0) for r0, r1, c0, c1, _ in LAST],
                    [smem, hbm], ring(D, TILE // 2, 1), 2 * block)(place, wd)
        got_d = [permute(c, to_block if i > 1 and LAST[i - 2][4] else to_x) for i, c in enumerate(cuts)]
        side = [permute(w, to_core) for w in (wg, wu, wd)]
        w13, w2 = call(own_kernel, (shape(slots, D, 2 * F), shape(slots, F, D)),
                       [smem] + [hbm] * 6, ring(F, TILE) + ring(D, TILE // 4), 6 * block)(place, wg, wu, wd, *side)

        def later(kernel, dest, got, out, cols, tile, rel_in=hbm):
            rel = permute(got, to_relay)
            return call(functools.partial(kernel, dest), shape(*out.shape), [smem, hbm, rel_in, hbm],
                        ring(cols, tile), 3 * got.size * 2, {3: 0}, cols)(place, got, rel, out)

        w13 = later(both_kernel, lambda o, j: half(o, j, 0), got_g, w13, F, TILE)
        w13 = later(both_kernel, lambda o, j: half(o, j, 1), got_u, w13, F, TILE)
        w2 = later(both_kernel, lambda o, j: rows_of(o, j, 0), got_d[0], w2, D, TILE // 4)
        w2 = later(first_kernel, lambda o, j: rows_of(o, j, BOTH_ROWS), got_d[1], w2, D, TILE // 2,
                   vmem)
        for i, got in enumerate(got_d[2:]):
            r0, r1, c0, c1, _ = LAST[i]

            def rect(out, j, r0=r0, r1=r1, c0=c0, c1=c1):
                return out.at[j, pl.ds(r0, r1 - r0), pl.ds(c0, c1 - c0)]

            w2 = call(functools.partial(last_kernel, rect),
                      shape(*w2.shape), [vmem, vmem, hbm], [pltpu.SemaphoreType.DMA((slots,))],
                      3 * got.size * 2, {2: 0})(place, got, w2)
        return w13[None], w2[None]

    spec_in = P(None, "ep", None, None)
    spec_out = P(None, ("dp", "ep"), None, None)
    return jax.shard_map(hand_over, mesh=mesh,
                         in_specs=(spec_in, spec_in, spec_in, P(None, None)),
                         out_specs=(spec_out, spec_out), check_vma=False)
```
